32 devices in a mesh: grp: 8 (over z, x), sp: 4 (over y, core).
Axes of the slice: x: 2, y: 2, z: 4, core: 2. Of those that a mesh axis runs over, the one named last changes fastest.
Arguments:
- query_rows: bfloat16 [4096, 4096], P(('grp', 'sp')), parts along dimension 0, may hold values from -250 to 250
- key_rows: bfloat16 [4096, 1024], P(('grp', 'sp')), parts along dimension 0, may hold values from -4 to 4
- value_rows: bfloat16 [4096, 1024], P(('grp', 'sp')), parts along dimension 0, may hold values from -6 to 6
- out_grad: bfloat16 [4096, 4096], P(('grp', 'sp')), parts along dimension 0, may hold values from -6 to 6
- question_lengths: int32 [64], P('grp'), parts along dimension 0, may hold values from 1 to 128, 256 in all
Outputs:
- query_grad: bfloat16 [4096, 4096], P(('grp', 'sp')), parts along dimension 0
- key_grad: bfloat16 [4096, 1024], P(('grp', 'sp')), parts along dimension 0
- value_grad: bfloat16 [4096, 1024], P(('grp', 'sp')), parts along dimension 0
The draws below stay inside these ranges and needn't reach their ends.
There are 8 independent parts, one for each index of `grp`. The reference program is written for one: setup_inputs(seed, part) draws one part's arguments, and reference() takes and returns one part's arrays. A program takes and returns all parts, laid end to end along the dimension named above; each array names one. Nothing has to cross between parts.
All inputs are finite; a program needn't handle non-finite values.
Results may differ from the reference program's by a relative error of at most 0.033.
Values may be sent and summed in bfloat16 or wider, within the bound.
No kernel may reach another device: no remote copies, remote signals or barrier semaphores. Data moves between devices by JAX's collectives and lax.ppermute only.
A program may use at most 128 MiB of HBM per device.

```python
import math
import jax
import jax.numpy as jnp
import numpy as np
from jax import lax

HD = 128
QH = 32
KVH = 8
SEQ = 512
DOC = 256
QMAX = 128
NQ = 8
BLK = 512


def joint_rows(key):
    folded = jax.random.fold_in(key, 11)
    query_key, keys_key = jax.random.split(folded, 2)
    queries = jnp.clip(jax.random.normal(query_key, (SEQ, QH * HD), jnp.float32), -4.0, 4.0)
    keyset = jnp.clip(jax.random.normal(keys_key, (SEQ, KVH * HD), jnp.float32), -4.0, 4.0)
    return (queries, keyset)


def draw_query_rows(key, part):
    return joint_rows(key)[0].astype(jnp.bfloat16)


def draw_key_rows(key, part):
    return joint_rows(key)[1].astype(jnp.bfloat16)


def steps_of(stream_key, extent, pieces, least, high):
    loudness, own = 1.0, jax.random.fold_in(stream_key, 6)
    for axis_at, shards_of in pieces:
        steps = jnp.exp(jax.random.uniform(jax.random.fold_in(own, axis_at), (shards_of,), jnp.float32, least / len(pieces), high / len(pieces)))
        loudness = loudness * jnp.repeat(steps, extent[axis_at] // shards_of).reshape([-1 if axis == axis_at else 1 for axis in range(len(extent))])
    return loudness


def length_profile(count, total, most, lean):
    weights = [(1 << 20) // math.isqrt(rank ** lean) + 1 for rank in range(2, count + 1)]
    surplus, counts = total - most - (count - 1), [1] * (count - 1)
    while surplus > 0:
        movable = [i for i in range(count - 1) if counts[i] < most]
        whole, left = sum([weights[i] for i in movable]), surplus
        for i in movable:
            more = min(most - counts[i], max(1, left * weights[i] // whole), surplus)
            counts[i] = counts[i] + more
            surplus = surplus - more
    return np.array([most] + counts)


def uneven(rng, count, total, bound, slope):
    if count == 2:
        one = jax.random.randint(rng, (), max(1, total - bound), min(bound, total - 1) + 1)
        return jnp.stack([one, total - one])
    sizes = jnp.asarray(length_profile(count, total, bound, slope), jnp.int32)
    couples = (count - 1) // 2
    giver, taker = sizes[1:1 + 2 * couples:2], sizes[2:2 + 2 * couples:2]
    slack = jnp.minimum(giver - 1, bound - taker)
    shifted = jax.random.randint(jax.random.fold_in(rng, 1), (couples,), 0, 1 << 20) % (slack + 1)
    sizes = sizes.at[1:1 + 2 * couples:2].set(giver - shifted).at[2:2 + 2 * couples:2].set(taker + shifted)
    return sizes[jax.random.permutation(jax.random.fold_in(rng, 2), count)]


def gaussian(rng, extent, spread, bound, cuts=(), held_as=jnp.bfloat16):
    level = steps_of(rng, extent, cuts, -0.22, 0.18) if cuts else 1.0
    values = jax.random.normal(rng, extent, jnp.float32) * spread * level
    return jnp.minimum(jnp.maximum(values, -bound), bound).astype(held_as)


def setup_inputs(seed: int = 0, part: int = 0) -> dict:
    seeds = jax.random.split(jax.random.key(seed), 6)
    part_splits = jax.random.split(jax.random.fold_in(seeds[5], part), 6)
    query_rows = draw_query_rows(jax.random.fold_in(jax.random.fold_in(seeds[5], part), 71), part)
    key_rows = draw_key_rows(jax.random.fold_in(jax.random.fold_in(seeds[5], part), 71), part)
    value_rows = gaussian(part_splits[2], (SEQ, KVH * HD), 1.0, 6.0, ((0, 4),))
    out_grad = gaussian(part_splits[3], (SEQ, QH * HD), 1.0, 6.0, ((0, 4),))
    question_lengths = uneven(part_splits[4], NQ, SEQ - DOC, QMAX, 2).astype(jnp.int32)
    return dict(query_rows=query_rows, key_rows=key_rows, value_rows=value_rows, out_grad=out_grad, question_lengths=question_lengths)


MASKED = -1e+30

def rounded(values):
    return lax.optimization_barrier(values.astype(jnp.bfloat16)).astype(jnp.float32)

def segment_ids(question_lengths):
    ends = jnp.cumsum(question_lengths).astype(jnp.int32)
    places = jnp.arange(SEQ, dtype=jnp.int32)
    inside = lax.optimization_barrier(jnp.sum((ends[None, :] <= (places - DOC)[:, None]).astype(jnp.int32), axis=1))
    return jnp.where(places < DOC, -1, inside).astype(jnp.int32)

def reference(query_rows, key_rows, value_rows, out_grad, question_lengths):
    segment = segment_ids(question_lengths)
    places = jnp.arange(SEQ, dtype=jnp.int32)
    group = QH // KVH
    scaling = 1.0 / math.sqrt(HD)
    block_count = SEQ // BLK
    queries = query_rows.reshape(SEQ, KVH, group, HD).transpose(1, 0, 2, 3)
    grads = out_grad.reshape(SEQ, KVH, group, HD).transpose(1, 0, 2, 3)
    keys = key_rows.reshape(SEQ, KVH, HD).transpose(1, 0, 2)
    values = value_rows.reshape(SEQ, KVH, HD).transpose(1, 0, 2)

    def one_group(packed):
        query_group, grad_group, key_group, value_group = packed
        key_float = key_group.astype(jnp.float32)
        value_float = value_group.astype(jnp.float32)

        def step(carry, block):
            key_sum, value_sum = carry
            start = (block * BLK).astype(jnp.int32)
            query_block = lax.dynamic_slice_in_dim(query_group, start, BLK, 0).astype(jnp.float32)
            grad_block = lax.dynamic_slice_in_dim(grad_group, start, BLK, 0).astype(jnp.float32)
            row_places = lax.dynamic_slice_in_dim(places, start, BLK, 0)
            row_segment = lax.dynamic_slice_in_dim(segment, start, BLK, 0)
            visible = (places[None, :] <= row_places[:, None]) & ((places[None, :] < DOC) | (segment[None, :] == row_segment[:, None]))
            scores = jnp.einsum('bgd,sd->gbs', query_block, key_float) * scaling
            scores = jnp.where(visible[None], scores, MASKED)
            peak = lax.optimization_barrier(jnp.max(scores, axis=2))
            log_total = peak + jnp.log(lax.optimization_barrier(jnp.sum(jnp.exp(scores - peak[..., None]), axis=2)))
            probs = jnp.exp(scores - log_total[..., None])
            probs_b = rounded(probs)
            output = rounded(jnp.einsum('gbs,sd->bgd', probs_b, value_float))
            delta = lax.optimization_barrier(jnp.sum(grad_block * output, axis=2)).T
            value_sum = value_sum + jnp.einsum('gbs,bgd->sd', probs_b, grad_block)
            prob_grad = jnp.einsum('bgd,sd->gbs', grad_block, value_float)
            score_grad = rounded(probs * (prob_grad - delta[..., None]))
            query_part = (jnp.einsum('gbs,sd->bgd', score_grad, key_float) * scaling).astype(jnp.bfloat16)
            key_sum = key_sum + jnp.einsum('gbs,bgd->sd', score_grad, query_block) * scaling
            return ((key_sum, value_sum), query_part)
        empty = jnp.zeros((SEQ, HD), jnp.float32)
        sums, query_parts = lax.scan(step, (empty, empty), jnp.arange(block_count, dtype=jnp.int32))
        return (query_parts.reshape(SEQ, group, HD), sums[0].astype(jnp.bfloat16), sums[1].astype(jnp.bfloat16))
    query_all, key_all, value_all = lax.map(one_group, (queries, grads, keys, values))
    query_grad = query_all.transpose(1, 0, 2, 3).reshape(SEQ, QH * HD)
    key_grad = key_all.transpose(1, 0, 2).reshape(SEQ, KVH * HD)
    value_grad = value_all.transpose(1, 0, 2).reshape(SEQ, KVH * HD)
    return (query_grad, key_grad, value_grad)
```

```python
from functools import partial
from functools import reduce
import math

import jax
import jax.numpy as jnp
from jax import lax
from jax.experimental import pallas as pl
from jax.experimental.pallas import tpu as pltpu
from jax.sharding import PartitionSpec as P

HD = 128
QH = 32
KVH = 8

CHUNKS = 2
TWO_WAY = True
VMEM_BYTES = 32 * 1024 * 1024


MASKED = -1e30


def widen(rows, copies):
    tokens = rows.shape[0]
    shaped = rows.reshape(tokens, KVH, 1, HD)
    return jnp.broadcast_to(shaped, (tokens, KVH, copies, HD)).reshape(tokens, KVH * copies * HD)


def segment_ids(question_lengths, length, doc_len):
    ends = jnp.cumsum(question_lengths)
    places = jnp.arange(length, dtype=jnp.int32)
    inside = jnp.sum((ends[None, :] <= (places - doc_len)[:, None]).astype(jnp.int32), axis=1)
    return jnp.where(places < doc_len, -1, inside)


def make_scores(query_block, key_block, visible, scaling):
    raw = (
        jnp.einsum("bkgd,skd->kgbs", query_block, key_block, preferred_element_type=jnp.float32)
        * scaling
    )
    return jnp.where(visible[None, None], raw, MASKED)


def weighted_values(probs_b, value_block):
    return jnp.einsum("kgbs,skd->bkgd", probs_b, value_block, preferred_element_type=jnp.float32)


def backward_block(probs, probs_b, delta, grad_block, query_block, key_block, value_block, scaling):
    value_part = jnp.einsum(
        "kgbs,bkgd->skd", probs_b, grad_block, preferred_element_type=jnp.float32
    )
    prob_grad = jnp.einsum(
        "bkgd,skd->kgbs", grad_block, value_block, preferred_element_type=jnp.float32
    )
    score_grad = (probs * (prob_grad - delta[..., None])).astype(jnp.bfloat16)
    query_part = jnp.einsum(
        "kgbs,skd->bkgd", score_grad, key_block, preferred_element_type=jnp.float32
    )
    key_part = (
        jnp.einsum("kgbs,bkgd->skd", score_grad, query_block, preferred_element_type=jnp.float32)
        * scaling
    )
    return (query_part, key_part, value_part)


def on_device(query_rows, key_rows, value_rows, out_grad, question_lengths):
    devices = lax.axis_size("sp")
    tokens = query_rows.shape[0]
    length = tokens * devices
    doc_len = length // 2
    block_len = min(512, length)
    block_count = length // block_len
    scaling = 1.0 / math.sqrt(HD)
    copies = max(KVH, devices) // KVH
    keys_local, values_local = (
        lax.all_to_all(widen(key_rows, copies), "sp", split_axis=1, concat_axis=0, tiled=True),
        lax.all_to_all(widen(value_rows, copies), "sp", split_axis=1, concat_axis=0, tiled=True),
    )
    queries_local, grads_local = (
        lax.all_to_all(query_rows, "sp", split_axis=1, concat_axis=0, tiled=True),
        lax.all_to_all(out_grad, "sp", split_axis=1, concat_axis=0, tiled=True),
    )
    key_heads = KVH * copies // devices
    per_group = QH // devices // key_heads
    queries = queries_local.reshape(length, key_heads, per_group, HD)
    grads = grads_local.reshape(length, key_heads, per_group, HD)
    keys = keys_local.reshape(length, key_heads, HD)
    values = values_local.reshape(length, key_heads, HD)
    segment = segment_ids(question_lengths, length, doc_len)
    places = jnp.arange(length, dtype=jnp.int32)
    query_shape = (block_len, key_heads, per_group, HD)
    key_shape = (block_len, key_heads, HD)
    key_sums = [jnp.zeros(key_shape, jnp.float32)] * block_count
    value_sums = [jnp.zeros(key_shape, jnp.float32)] * block_count
    query_parts = []
    for row_block in range(block_count):
        row_start = row_block * block_len
        query_block = queries[row_start : row_start + block_len]
        grad_block = grads[row_start : row_start + block_len]
        row_places = places[row_start : row_start + block_len]
        row_segment = segment[row_start : row_start + block_len]
        needs = []
        scores = []
        for col_block in range(row_block + 1):
            col_start = col_block * block_len
            col_places = places[col_start : col_start + block_len]
            col_segment = segment[col_start : col_start + block_len]
            visible = (col_places[None, :] <= row_places[:, None]) & (
                (col_places[None, :] < doc_len) | (col_segment[None, :] == row_segment[:, None])
            )
            needed = True
            needs.append(needed)
            scores.append(
                make_scores(query_block, keys[col_start : col_start + block_len], visible, scaling)
            )
        peak = reduce(jnp.maximum, [jnp.max(score, axis=3) for score in scores])
        total = reduce(
            jnp.add, [jnp.sum(jnp.exp(score - peak[..., None]), axis=3) for score in scores]
        )
        log_total = peak + jnp.log(total)
        probs = [jnp.exp(score - log_total[..., None]) for score in scores]
        probs_low = [single.astype(jnp.bfloat16) for single in probs]
        output = jnp.zeros(query_shape, jnp.float32)
        for col_block in range(row_block + 1):
            col_start = col_block * block_len
            output = output + weighted_values(
                probs_low[col_block], values[col_start : col_start + block_len]
            )
        output_low = output.astype(jnp.bfloat16)
        delta = jnp.einsum(
            "bkgd,bkgd->kgb", grad_block, output_low, preferred_element_type=jnp.float32
        )
        query_sum = jnp.zeros(query_shape, jnp.float32)
        for col_block in range(row_block + 1):
            col_start = col_block * block_len
            action = partial(
                backward_block,
                probs[col_block],
                probs_low[col_block],
                delta,
                grad_block,
                query_block,
                keys[col_start : col_start + block_len],
                values[col_start : col_start + block_len],
                scaling,
            )
            query_part, key_part, value_part = action()
            query_sum = query_sum + query_part
            key_sums[col_block] = key_sums[col_block] + key_part
            value_sums[col_block] = value_sums[col_block] + value_part
        query_parts.append((query_sum * scaling).astype(jnp.bfloat16))
    query_local = jnp.concatenate(query_parts, axis=0).reshape(length, key_heads * per_group * HD)
    key_local = jnp.concatenate(key_sums, axis=0).reshape(length, key_heads * HD)
    value_local = jnp.concatenate(value_sums, axis=0).reshape(length, key_heads * HD)
    query_grad = lax.all_to_all(query_local, "sp", split_axis=0, concat_axis=1, tiled=True)
    key_back, value_back = (
        lax.all_to_all(key_local, "sp", split_axis=0, concat_axis=1, tiled=True),
        lax.all_to_all(value_local, "sp", split_axis=0, concat_axis=1, tiled=True),
    )
    key_grad = (
        jnp.sum(key_back.reshape(tokens, KVH, copies, HD), axis=2)
        .reshape(tokens, KVH * HD)
        .astype(jnp.bfloat16)
    )
    value_grad = (
        jnp.sum(value_back.reshape(tokens, KVH, copies, HD), axis=2)
        .reshape(tokens, KVH * HD)
        .astype(jnp.bfloat16)
    )
    return (query_grad, key_grad, value_grad)


LOG2E = 1.4426950408889634
HIDDEN = -1e30


def contract(left, right, left_dim, right_dim):
    return lax.dot_general(
        left, right, (((left_dim,), (right_dim,)), ((), ())), preferred_element_type=jnp.float32
    )


def pack_kernel(place, keys, values, *sends):
    core = place[0] % 2
    chunks = len(sends) // 2
    group_cols = keys.shape[1] // 2
    heads = group_cols // HD // chunks
    for side in range(2):
        base = (core if side == 0 else 1 - core) * group_cols
        for chunk in range(chunks):
            for head in range(heads):
                start = pl.multiple_of(base + (chunk * heads + head) * HD, HD)
                out = sends[side * chunks + chunk]
                out[:, head * 2 * HD : head * 2 * HD + HD] = keys[:, pl.ds(start, HD)]
                out[:, head * 2 * HD + HD : (head + 1) * 2 * HD] = values[:, pl.ds(start, HD)]


def attend_kernel(
    chunk, heads, place, lengths,
    q_own, q_sib, g_own, g_sib, k_own, k_sib, v_own, v_sib, far_same, far_cross,
    dq_own, dq_sib, near_own, near_sib, out_same, out_cross, bias,
):
    core = place[0] % 2
    asking = place[0] // 2
    first = core == 0
    rows = q_own.shape[0]
    group = QH // KVH
    scaling = 1.0 / math.sqrt(HD)
    power = scaling * LOG2E
    asks = asking == 1

    def ordered(own, sib):
        return jnp.where(first, own, sib), jnp.where(first, sib, own)

    spots = lax.broadcasted_iota(jnp.int32, (2 * rows, 2 * rows), 1)
    key_spots = lax.broadcasted_iota(jnp.int32, (2 * rows, 2 * rows), 0)
    begin = jnp.zeros((1, 2 * rows), jnp.int32)
    spot_row = lax.broadcasted_iota(jnp.int32, (1, 2 * rows), 1)
    end = jnp.int32(0)
    for question in range(lengths.shape[0]):
        end = end + lengths[question]
        begin = begin + jnp.where(spot_row >= end, lengths[question], 0)
    begin = begin * asking
    bias[...] = jnp.where((key_spots <= spots) & (key_spots >= begin), 0.0, HIDDEN)

    key_base = core * (k_own.shape[1] // 2)
    query_base = core * (q_own.shape[1] // 2)
    for head in range(heads):
        local = chunk * heads + head
        key_at = pl.multiple_of(key_base + local * HD, HD)
        k_lo, k_hi = ordered(k_own[:, pl.ds(key_at, HD)], k_sib[:, pl.ds(key_at, HD)])
        v_lo, v_hi = ordered(v_own[:, pl.ds(key_at, HD)], v_sib[:, pl.ds(key_at, HD)])
        far = head * 2 * HD
        keys = jnp.concatenate(
            [far_same[:, far : far + HD], far_cross[:, far : far + HD], k_lo, k_hi], axis=0
        )
        values = jnp.concatenate(
            [far_same[:, far + HD : far + 2 * HD], far_cross[:, far + HD : far + 2 * HD], v_lo, v_hi],
            axis=0,
        )
        keys_t = keys.T
        dk_lo = dv_lo = dk_hi = dv_hi = None
        for pair in range(group // 2):
            q_parts, g_parts = [], []
            for member in range(2):
                at = pl.multiple_of(query_base + (local * group + pair * 2 + member) * HD, HD)
                q_parts.append(ordered(q_own[:, pl.ds(at, HD)], q_sib[:, pl.ds(at, HD)]))
                g_parts.append(ordered(g_own[:, pl.ds(at, HD)], g_sib[:, pl.ds(at, HD)]))
            dq = []
            for side in range(2):
                q = jnp.concatenate([q_parts[0][side], q_parts[1][side]], axis=0)
                g = jnp.concatenate([g_parts[0][side], g_parts[1][side]], axis=0)
                near = (side + 1) * rows
                count = 2 * rows + near
                scores = contract(keys[:count], q, 1, 1)
                prob_grad = contract(values[:count], g, 1, 1)
                hide = bias[:near, side * rows : (side + 1) * rows]
                hide = jnp.concatenate([hide, hide], axis=1)
                s_far = scores[: 2 * rows]
                s_near = scores[2 * rows :] + hide
                peak = jnp.max(s_near, axis=0, keepdims=True)
                peak = jnp.maximum(
                    peak, jnp.where(asks, jnp.max(s_far, axis=0, keepdims=True), HIDDEN)
                )
                e_far = jnp.exp2((s_far - jnp.where(asks, peak, -HIDDEN)) * power)
                e_near = jnp.exp2((s_near - peak) * power)
                exps = jnp.concatenate([e_far, e_near], axis=0)
                probs = exps * (1.0 / jnp.sum(exps, axis=0, keepdims=True))
                delta = jnp.sum(probs * prob_grad, axis=0, keepdims=True)
                score_grad = (probs * (prob_grad - delta)).astype(jnp.bfloat16)
                dv = contract(probs.astype(jnp.bfloat16), g, 1, 0)
                dk = contract(score_grad, q, 1, 0)
                if side == 0:
                    dk_lo = dk if dk_lo is None else dk_lo + dk
                    dv_lo = dv if dv_lo is None else dv_lo + dv
                else:
                    dk_hi = dk if dk_hi is None else dk_hi + dk
                    dv_hi = dv if dv_hi is None else dv_hi + dv
                dq_t = contract(keys_t[:, :count], score_grad, 1, 0) * scaling
                dq.append(dq_t.T.astype(jnp.bfloat16))
            for member in range(2):
                at = (head * group + pair * 2 + member) * HD
                low = dq[0][member * rows : (member + 1) * rows]
                high = dq[1][member * rows : (member + 1) * rows]
                dq_own[:, at : at + HD] = jnp.where(first, low, high)
                dq_sib[:, at : at + HD] = jnp.where(first, high, low)
        for slot, (low, high) in enumerate(((dk_lo, dk_hi), (dv_lo, dv_hi))):
            size = scaling if slot == 0 else 1.0
            at = far + slot * HD
            near = (low[2 * rows :] + high[2 * rows : 3 * rows]) * size
            last = high[3 * rows :] * size
            near_own[:, at : at + HD] = jnp.where(first, near, last)
            near_sib[:, at : at + HD] = jnp.where(first, last, near).astype(near_sib.dtype)
            distant = ((low[: 2 * rows] + high[: 2 * rows]) * size).astype(out_same.dtype)
            out_same[:, at : at + HD] = distant[:rows]
            out_cross[:, at : at + HD] = distant[rows:]


def join_queries_kernel(chunks, place, *refs):
    core = place[0] % 2
    out = refs[-1]
    width = out.shape[1] // 2 // chunks
    for side in range(2):
        base = (core if side == 0 else 1 - core) * (out.shape[1] // 2)
        for chunk in range(chunks):
            at = pl.multiple_of(base + chunk * width, HD)
            out[:, pl.ds(at, width)] = refs[side * chunks + chunk][...]


def join_keys_kernel(chunks, place, *refs):
    core = place[0] % 2
    told = place[0] // 2 == 0
    dk, dv = refs[-2:]
    width = dk.shape[1] // 2
    heads = width // HD // chunks
    for side in range(2):
        base = (core if side == 0 else 1 - core) * width
        for chunk in range(chunks):
            near = refs[side * chunks + chunk]
            distant = refs[(2 + side) * chunks + chunk]
            total = near[...].astype(jnp.float32) + jnp.where(
                told, distant[...].astype(jnp.float32), 0.0
            )
            for head in range(heads):
                at = pl.multiple_of(base + (chunk * heads + head) * HD, HD)
                first = head * 2 * HD
                dk[:, pl.ds(at, HD)] = total[:, first : first + HD].astype(dk.dtype)
                dv[:, pl.ds(at, HD)] = total[:, first + HD : first + 2 * HD].astype(dv.dtype)


def local_call(kernel, outs, args, scalars, name, scratch=(), flops=0):
    specs = [pl.BlockSpec(memory_space=pltpu.SMEM)] * scalars
    specs += [pl.BlockSpec(memory_space=pltpu.VMEM)] * (len(args) - scalars)
    return pl.pallas_call(
        kernel,
        out_shape=tuple(outs),
        in_specs=specs,
        out_specs=tuple(pl.BlockSpec(memory_space=pltpu.VMEM) for _ in outs),
        scratch_shapes=scratch,
        compiler_params=pltpu.CompilerParams(vmem_limit_bytes=VMEM_BYTES),
        cost_estimate=pl.CostEstimate(flops=flops, transcendentals=0, bytes_accessed=0),
        name=name,
    )(*args)


def on_pair(query_rows, key_rows, value_rows, out_grad, question_lengths):
    rows = query_rows.shape[0]
    place = lax.axis_index("sp").astype(jnp.int32).reshape(1)
    chunks = CHUNKS
    heads = KVH // 2 // chunks
    group = QH // KVH
    bf16 = jnp.bfloat16
    sib = [(0, 1), (1, 0), (2, 3), (3, 2)]
    same = [(0, 2), (1, 3)]
    cross = [(0, 3), (1, 2)]
    back_same = [(2, 0), (3, 1)]
    back_cross = [(3, 0), (2, 1)]
    if TWO_WAY:
        same = back_same = same + back_same
        cross = back_cross = cross + back_cross
    send = lambda value, perm: lax.ppermute(value, "sp", perm)
    packs = local_call(
        pack_kernel,
        [jax.ShapeDtypeStruct((rows, heads * 2 * HD), bf16)] * (2 * chunks),
        (place, key_rows, value_rows), 1, "pack",
    )
    far_same = [send(packs[c], same) for c in range(chunks)]
    far_cross = [send(packs[chunks + c], cross) for c in range(chunks)]
    k_sib, v_sib = send(key_rows, sib), send(value_rows, sib)
    q_sib, g_sib = send(query_rows, sib), send(out_grad, sib)
    shape = jax.ShapeDtypeStruct
    dq_own, dq_sib, near_own, near_sib, told_same, told_cross = [], [], [], [], [], []
    for chunk in range(chunks):
        outs = local_call(
            partial(attend_kernel, chunk, heads),
            [
                shape((rows, heads * group * HD), bf16),
                shape((rows, heads * group * HD), bf16),
                shape((rows, heads * 2 * HD), jnp.float32),
                shape((rows, heads * 2 * HD), bf16),
                shape((rows, heads * 2 * HD), bf16),
                shape((rows, heads * 2 * HD), bf16),
            ],
            (
                place, question_lengths, query_rows, q_sib, out_grad, g_sib,
                key_rows, k_sib, value_rows, v_sib, far_same[chunk], far_cross[chunk],
            ),
            2, "attend", scratch=[pltpu.VMEM((2 * rows, 2 * rows), jnp.float32)],
            flops=heads * group * 10 * HD * 2 * rows * 4 * rows,
        )
        dq_own.append(outs[0])
        near_own.append(outs[2])
        told_same.append(send(outs[4], back_same))
        told_cross.append(send(outs[5], back_cross))
        dq_sib.append(send(outs[1], sib))
        near_sib.append(send(outs[3], sib))
    query_grad, = local_call(
        partial(join_queries_kernel, chunks), [shape(query_rows.shape, bf16)],
        (place, *dq_own, *dq_sib), 1, "join_queries",
    )
    key_grad, value_grad = local_call(
        partial(join_keys_kernel, chunks), [shape(key_rows.shape, bf16)] * 2,
        (place, *near_own, *near_sib, *told_same, *told_cross), 1, "join_keys",
    )
    return query_grad, key_grad, value_grad


def solution(mesh):
    return jax.shard_map(
        on_pair if mesh.shape["sp"] == 4 else on_device,
        mesh=mesh,
        in_specs=(
            P(("grp", "sp"), None),
            P(("grp", "sp"), None),
            P(("grp", "sp"), None),
            P(("grp", "sp"), None),
            P("grp"),
        ),
        out_specs=(P(("grp", "sp"), None), P(("grp", "sp"), None), P(("grp", "sp"), None)),
        check_vma=False,
    )
```

```python
from functools import partial
from functools import reduce
import math

import jax
import jax.numpy as jnp
from jax import lax
from jax.experimental import pallas as pl
from jax.experimental.pallas import tpu as pltpu
from jax.sharding import PartitionSpec as P

HD = 128
QH = 32
KVH = 8

LAG = 2
VMEM_BYTES = 32 * 1024 * 1024


MASKED = -1e30


def widen(rows, copies):
    tokens = rows.shape[0]
    shaped = rows.reshape(tokens, KVH, 1, HD)
    return jnp.broadcast_to(shaped, (tokens, KVH, copies, HD)).reshape(tokens, KVH * copies * HD)


def segment_ids(question_lengths, length, doc_len):
    ends = jnp.cumsum(question_lengths)
    places = jnp.arange(length, dtype=jnp.int32)
    inside = jnp.sum((ends[None, :] <= (places - doc_len)[:, None]).astype(jnp.int32), axis=1)
    return jnp.where(places < doc_len, -1, inside)


def make_scores(query_block, key_block, visible, scaling):
    raw = (
        jnp.einsum("bkgd,skd->kgbs", query_block, key_block, preferred_element_type=jnp.float32)
        * scaling
    )
    return jnp.where(visible[None, None], raw, MASKED)


def weighted_values(probs_b, value_block):
    return jnp.einsum("kgbs,skd->bkgd", probs_b, value_block, preferred_element_type=jnp.float32)


def backward_block(probs, probs_b, delta, grad_block, query_block, key_block, value_block, scaling):
    value_part = jnp.einsum(
        "kgbs,bkgd->skd", probs_b, grad_block, preferred_element_type=jnp.float32
    )
    prob_grad = jnp.einsum(
        "bkgd,skd->kgbs", grad_block, value_block, preferred_element_type=jnp.float32
    )
    score_grad = (probs * (prob_grad - delta[..., None])).astype(jnp.bfloat16)
    query_part = jnp.einsum(
        "kgbs,skd->bkgd", score_grad, key_block, preferred_element_type=jnp.float32
    )
    key_part = (
        jnp.einsum("kgbs,bkgd->skd", score_grad, query_block, preferred_element_type=jnp.float32)
        * scaling
    )
    return (query_part, key_part, value_part)


def on_device(query_rows, key_rows, value_rows, out_grad, question_lengths):
    devices = lax.axis_size("sp")
    tokens = query_rows.shape[0]
    length = tokens * devices
    doc_len = length // 2
    block_len = min(512, length)
    block_count = length // block_len
    scaling = 1.0 / math.sqrt(HD)
    copies = max(KVH, devices) // KVH
    keys_local, values_local = (
        lax.all_to_all(widen(key_rows, copies), "sp", split_axis=1, concat_axis=0, tiled=True),
        lax.all_to_all(widen(value_rows, copies), "sp", split_axis=1, concat_axis=0, tiled=True),
    )
    queries_local, grads_local = (
        lax.all_to_all(query_rows, "sp", split_axis=1, concat_axis=0, tiled=True),
        lax.all_to_all(out_grad, "sp", split_axis=1, concat_axis=0, tiled=True),
    )
    key_heads = KVH * copies // devices
    per_group = QH // devices // key_heads
    queries = queries_local.reshape(length, key_heads, per_group, HD)
    grads = grads_local.reshape(length, key_heads, per_group, HD)
    keys = keys_local.reshape(length, key_heads, HD)
    values = values_local.reshape(length, key_heads, HD)
    segment = segment_ids(question_lengths, length, doc_len)
    places = jnp.arange(length, dtype=jnp.int32)
    query_shape = (block_len, key_heads, per_group, HD)
    key_shape = (block_len, key_heads, HD)
    key_sums = [jnp.zeros(key_shape, jnp.float32)] * block_count
    value_sums = [jnp.zeros(key_shape, jnp.float32)] * block_count
    query_parts = []
    for row_block in range(block_count):
        row_start = row_block * block_len
        query_block = queries[row_start : row_start + block_len]
        grad_block = grads[row_start : row_start + block_len]
        row_places = places[row_start : row_start + block_len]
        row_segment = segment[row_start : row_start + block_len]
        scores = []
        for col_block in range(row_block + 1):
            col_start = col_block * block_len
            col_places = places[col_start : col_start + block_len]
            col_segment = segment[col_start : col_start + block_len]
            visible = (col_places[None, :] <= row_places[:, None]) & (
                (col_places[None, :] < doc_len) | (col_segment[None, :] == row_segment[:, None])
            )
            scores.append(
                make_scores(query_block, keys[col_start : col_start + block_len], visible, scaling)
            )
        peak = reduce(jnp.maximum, [jnp.max(score, axis=3) for score in scores])
        total = reduce(
            jnp.add, [jnp.sum(jnp.exp(score - peak[..., None]), axis=3) for score in scores]
        )
        log_total = peak + jnp.log(total)
        probs = [jnp.exp(score - log_total[..., None]) for score in scores]
        probs_low = [single.astype(jnp.bfloat16) for single in probs]
        output = jnp.zeros(query_shape, jnp.float32)
        for col_block in range(row_block + 1):
            col_start = col_block * block_len
            output = output + weighted_values(
                probs_low[col_block], values[col_start : col_start + block_len]
            )
        output_low = output.astype(jnp.bfloat16)
        delta = jnp.einsum(
            "bkgd,bkgd->kgb", grad_block, output_low, preferred_element_type=jnp.float32
        )
        query_sum = jnp.zeros(query_shape, jnp.float32)
        for col_block in range(row_block + 1):
            col_start = col_block * block_len
            action = partial(
                backward_block,
                probs[col_block],
                probs_low[col_block],
                delta,
                grad_block,
                query_block,
                keys[col_start : col_start + block_len],
                values[col_start : col_start + block_len],
                scaling,
            )
            query_part, key_part, value_part = action()
            query_sum = query_sum + query_part
            key_sums[col_block] = key_sums[col_block] + key_part
            value_sums[col_block] = value_sums[col_block] + value_part
        query_parts.append((query_sum * scaling).astype(jnp.bfloat16))
    query_local = jnp.concatenate(query_parts, axis=0).reshape(length, key_heads * per_group * HD)
    key_local = jnp.concatenate(key_sums, axis=0).reshape(length, key_heads * HD)
    value_local = jnp.concatenate(value_sums, axis=0).reshape(length, key_heads * HD)
    query_grad = lax.all_to_all(query_local, "sp", split_axis=0, concat_axis=1, tiled=True)
    key_back, value_back = (
        lax.all_to_all(key_local, "sp", split_axis=0, concat_axis=1, tiled=True),
        lax.all_to_all(value_local, "sp", split_axis=0, concat_axis=1, tiled=True),
    )
    key_grad = (
        jnp.sum(key_back.reshape(tokens, KVH, copies, HD), axis=2)
        .reshape(tokens, KVH * HD)
        .astype(jnp.bfloat16)
    )
    value_grad = (
        jnp.sum(value_back.reshape(tokens, KVH, copies, HD), axis=2)
        .reshape(tokens, KVH * HD)
        .astype(jnp.bfloat16)
    )
    return (query_grad, key_grad, value_grad)


LOG2E = 1.4426950408889634
HIDDEN = -1e30


def contract(left, right, left_dim, right_dim):
    return lax.dot_general(
        left, right, (((left_dim,), (right_dim,)), ((), ())), preferred_element_type=jnp.float32
    )


def start_all(pairs, sems):
    copies = [pltpu.make_async_copy(src, dst, sems.at[i]) for i, (src, dst) in enumerate(pairs)]
    for copy in copies:
        copy.start()
    return copies


def halves_into(sources, side, out):
    pairs, at = [], 0
    for source in sources:
        half = source.shape[1] // 2
        start = pl.multiple_of(side * half, HD)
        pairs.append((source.at[:, pl.ds(start, half)], out.at[:, at : at + half]))
        at += half
    return pairs


def pack_kernel(place, queries, grads, keys, values, *refs):
    *sends, sib_send, sems = refs
    core = place[0] % 2
    half = keys.shape[1] // 2
    pairs = []
    for index, out in enumerate(sends):
        chunk, side = index // 2, index % 2
        base = (core if side == 0 else 1 - core) * half
        start = pl.multiple_of(base + chunk * HD, HD)
        pairs.append((keys.at[:, pl.ds(start, HD)], out.at[:, :HD]))
        pairs.append((values.at[:, pl.ds(start, HD)], out.at[:, HD:]))
    pairs += halves_into((queries, grads, keys, values), 1 - core, sib_send)
    for copy in start_all(pairs, sems):
        copy.wait()


def stage_kernel(place, queries, grads, keys, values, lengths, own_all, bias, spans, sems):
    core = place[0] % 2
    asking = place[0] // 2
    pairs = [(lengths, spans)] + halves_into((queries, grads, keys, values), core, own_all)
    copies = start_all(pairs, sems)
    copies[0].wait()
    spots = lax.broadcasted_iota(jnp.int32, bias.shape, 1)
    key_spots = lax.broadcasted_iota(jnp.int32, bias.shape, 0)
    spot_row = lax.broadcasted_iota(jnp.int32, (1, bias.shape[1]), 1)
    begin = jnp.zeros((1, bias.shape[1]), jnp.int32)
    end = jnp.int32(0)
    for question in range(lengths.shape[0]):
        end = end + spans[question]
        begin = begin + jnp.where(spot_row >= end, spans[question], 0)
    begin = begin * asking
    bias[...] = jnp.where((key_spots <= spots) & (key_spots >= begin), 0.0, HIDDEN)
    for copy in copies[1:]:
        copy.wait()


def specialise(place, body):
    core, asking = place[0] % 2, place[0] // 2
    for first in (True, False):
        for asks in (True, False):
            @pl.when((core == (0 if first else 1)) & (asking == (1 if asks else 0)))
            def _(first=first, asks=asks):
                body(asks, (lambda own, sib: (own, sib)) if first else (lambda own, sib: (sib, own)))


def columns(own_all, head):
    group = QH // KVH
    heads = own_all.shape[1] // (2 * (group + 1) * HD)
    query_at, grad_at = head * group * HD, (heads + head) * group * HD
    key_at = (2 * heads * group + head) * HD
    return query_at, grad_at, key_at, key_at + heads * HD


def stacked(ref, at, pair):
    first = at + 2 * pair * HD
    return jnp.concatenate([ref[:, first : first + HD], ref[:, first + HD : first + 2 * HD]], axis=0)


def head_parts(asks, order, own_all, sib_all, far, key_at, value_at):
    near = order(own_all, sib_all)
    keys = [ref[:, key_at : key_at + HD] for ref in near]
    values = [ref[:, value_at : value_at + HD] for ref in near]
    if asks:
        distant = order(*far) if len(far) == 2 else far
        keys = [ref[:, :HD] for ref in distant] + keys
        values = [ref[:, HD:] for ref in distant] + values
    return near, jnp.concatenate(keys, axis=0), jnp.concatenate(values, axis=0)


def soften(keys, values, q, g, hide, distant, power):
    scores = contract(keys, q, 1, 1)
    prob_grad = contract(values, g, 1, 1)
    hide = jnp.concatenate([hide, hide], axis=1)
    if distant:
        scores = jnp.concatenate([scores[:distant], scores[distant:] + hide], axis=0)
    else:
        scores = scores + hide
    peak = jnp.max(scores, axis=0, keepdims=True)
    exps = jnp.exp2((scores - peak) * power)
    probs = exps * (1.0 / jnp.sum(exps, axis=0, keepdims=True))
    delta = jnp.sum(probs * prob_grad, axis=0, keepdims=True)
    score_grad = (probs * (prob_grad - delta)).astype(jnp.bfloat16)
    return probs.astype(jnp.bfloat16), score_grad


def accumulate(sums, slot, value):
    sums[slot] = value if sums[slot] is None else sums[slot] + value


def attend_kernel(unit, place, bias, own_all, sib_all, *refs):
    refs = list(refs)
    far = [refs.pop(0) for _ in range(unit["far"])]
    split = unit["told"] == 2
    outs = refs[-5 if not split else -7 :]
    dq_own, dq_sib, near_own, near_sib, out = outs[:5]
    head = unit["head"]
    rows = own_all.shape[0]
    group = QH // KVH
    scaling = 1.0 / math.sqrt(HD)
    power = scaling * LOG2E
    low = jnp.bfloat16
    query_at, grad_at, key_at, value_at = columns(own_all, head)

    def body(asks, order):
        if not asks and unit["later"] is not None:
            _, _, later_key, later_value = columns(own_all, unit["later"])
            for half, ref in enumerate(order(own_all, sib_all)):
                spot = slice(half * rows, (half + 1) * rows)
                out[spot, :HD] = ref[:, later_key : later_key + HD]
                out[spot, HD:] = ref[:, later_value : later_value + HD]
        distant = 2 * rows if asks else 0
        near, keys, values = head_parts(asks, order, own_all, sib_all, far, key_at, value_at)
        partial_only = split and asks
        keys_t = None if partial_only else keys.T
        dk, dv, told = [None, None], [None, None], [None, None]
        for pair in range(group // 2):
            for side in range(2):
                q = stacked(near[side], query_at, pair)
                g = stacked(near[side], grad_at, pair)
                count = distant + (side + 1) * rows
                hide = bias[: (side + 1) * rows, side * rows : (side + 1) * rows]
                probs, score_grad = soften(keys[:count], values[:count], q, g, hide, distant, power)
                if partial_only:
                    slot = pair * 2 + side
                    outs[5][slot, :count] = probs
                    outs[6][slot, :count] = score_grad
                    wanted = order(0, rows)[0]
                    accumulate(told, 0, contract(score_grad[wanted : wanted + rows], q, 1, 0))
                    accumulate(told, 1, contract(probs[wanted : wanted + rows], g, 1, 0))
                    continue
                accumulate(dv, side, contract(probs, g, 1, 0))
                accumulate(dk, side, contract(score_grad, q, 1, 0))
                dq = (contract(keys_t[:, :count], score_grad, 1, 0) * scaling).T.astype(low)
                target = order(dq_own, dq_sib)[side]
                for member in range(2):
                    at = (pair * 2 + member) * HD
                    target[:, at : at + HD] = dq[member * rows : (member + 1) * rows]
        if partial_only:
            out[:, :HD] = (told[0] * scaling).astype(low)
            out[:, HD:] = told[1].astype(low)
            return
        for slot, (lo, hi) in enumerate((dk, dv)):
            size = scaling if slot == 0 else 1.0
            spot = slice(slot * HD, (slot + 1) * HD)
            first, second = order(near_own, near_sib)
            first[:, spot] = (lo[distant:] + hi[distant : distant + rows]) * size
            second[:, spot] = hi[distant + rows :] * size
            if asks:
                out[:, spot] = ((lo[:distant] + hi[:distant]) * size).astype(low)

    specialise(place, body)


def settle_kernel(unit, place, own_all, sib_all, *refs):
    refs = list(refs)
    far = [refs.pop(0) for _ in range(unit["far"])]
    dq_own_in, dq_sib_in, near_own_in, near_sib_in, probs_in, grads_in = refs[:6]
    dq_own, back, near_own, out = refs[6:]
    rows = own_all.shape[0]
    group = QH // KVH
    scaling = 1.0 / math.sqrt(HD)
    low = jnp.bfloat16
    query_at, grad_at, key_at, value_at = columns(own_all, unit["head"])

    def body(asks, order):
        if not asks:
            dq_own[...] = dq_own_in[...]
            near_own[...] = near_own_in[...]
            back[:, : group * HD] = dq_sib_in[...]
            back[:, group * HD :] = near_sib_in[...].astype(low)
            return
        near, keys, _ = head_parts(asks, order, own_all, sib_all, far, key_at, value_at)
        keys_t = keys.T
        distant = 2 * rows
        dk, dv, told = [None, None], [None, None], [None, None]
        for pair in range(group // 2):
            for side in range(2):
                slot = pair * 2 + side
                count = distant + (side + 1) * rows
                q = stacked(near[side], query_at, pair)
                g = stacked(near[side], grad_at, pair)
                probs, score_grad = probs_in[slot, :count], grads_in[slot, :count]
                wanted = order(0, rows)[1]
                accumulate(told, 0, contract(score_grad[wanted : wanted + rows], q, 1, 0))
                accumulate(told, 1, contract(probs[wanted : wanted + rows], g, 1, 0))
                accumulate(dv, side, contract(probs[distant:], g, 1, 0))
                accumulate(dk, side, contract(score_grad[distant:], q, 1, 0))
                dq = (contract(keys_t[:, :count], score_grad, 1, 0) * scaling).T.astype(low)
                target = order(dq_own, back)[side]
                for member in range(2):
                    at = (pair * 2 + member) * HD
                    target[:, at : at + HD] = dq[member * rows : (member + 1) * rows]
        for slot, (lo, hi) in enumerate((dk, dv)):
            size = scaling if slot == 0 else 1.0
            at = slot * HD
            targets = order((near_own, at), (back, group * HD + at))
            for (target, spot), value in zip(targets, (lo + hi[:rows], hi[rows:])):
                target[:, spot : spot + HD] = (value * size).astype(target.dtype)
            out[:, at : at + HD] = (told[slot] * size).astype(low)

    specialise(place, body)


def fold_kernel(count, place, *refs):
    nears, tolds, back = refs[:count], refs[count : 2 * count], refs[-1]
    core = place[0] % 2
    hears = place[0] // 2 == 0
    rows, width = nears[0].shape
    at = pl.multiple_of((1 - core) * rows, rows)
    for index in range(count):
        told = jnp.where(hears, tolds[index][pl.ds(at, rows), :].astype(jnp.float32), 0.0)
        back[:, index * width : (index + 1) * width] = (nears[index][...] + told).astype(back.dtype)


def join_kernel(units, place, *refs):
    outs, (sums, sems) = refs[-5:-2], refs[-2:]
    core = place[0] % 2
    hears = place[0] // 2 == 0
    group = QH // KVH
    halves = [out.shape[1] // 2 for out in outs]
    amount = len(units)
    late = units[0]["told"] == 2
    copies = []

    def write(source, out, start, width):
        target = out.at[:, pl.ds(pl.multiple_of(start, HD), width)]
        copies.append(pltpu.make_async_copy(source, target, sems.at[len(copies)]))
        copies[-1].start()

    for index, unit in enumerate(units):
        width = group * HD
        at = unit["head"] * width
        sib_part = refs[amount + index]
        write(refs[index], outs[0], core * halves[0] + at, width)
        write(sib_part.at[:, :width], outs[0], (1 - core) * halves[0] + at, width)
    own_rows = pl.multiple_of(core * refs[0].shape[0], HD)
    for index, unit in enumerate(units):
        near, told = refs[2 * amount + index], refs[3 * amount + index]
        rows = near.shape[0]
        heard = told[...] if late else told[pl.ds(own_rows, rows), :]
        total = near[...] + jnp.where(hears, heard.astype(jnp.float32), 0.0)
        sums[index] = total.astype(sums.dtype)
        for slot in range(2):
            start = core * halves[1] + unit["head"] * HD
            write(sums.at[index, :, slot * HD : (slot + 1) * HD], outs[1 + slot], start, HD)
    other = refs[4 * amount]
    if late:
        told = refs[4 * amount + 1]
        rows = told.shape[0]
        total = other[:, group * HD :].astype(jnp.float32) + jnp.where(
            hears, told[...].astype(jnp.float32), 0.0
        )
        sums[amount] = total.astype(sums.dtype)
        other = sums.at[amount]
    for index, unit in enumerate(units):
        for slot in range(2):
            start = (1 - core) * halves[1] + unit["head"] * HD
            at = (2 * index + slot) * HD
            write(other.at[:, at : at + HD], outs[1 + slot], start, HD)
    for copy in copies:
        copy.wait()


def local_call(kernel, outs, args, scratch=(), flops=0, space=pltpu.VMEM, aliases=None, out_space=pltpu.VMEM, in_spaces=None):
    specs = [pl.BlockSpec(memory_space=pltpu.SMEM)]
    specs += [pl.BlockSpec(memory_space=kind) for kind in in_spaces or [space] * (len(args) - 1)]
    return pl.pallas_call(
        kernel,
        out_shape=tuple(outs),
        in_specs=specs,
        out_specs=tuple(pl.BlockSpec(memory_space=out_space) for _ in outs),
        scratch_shapes=scratch,
        input_output_aliases=aliases or {},
        compiler_params=pltpu.CompilerParams(vmem_limit_bytes=VMEM_BYTES),
        cost_estimate=pl.CostEstimate(flops=flops, transcendentals=0, bytes_accessed=0),
    )(*args)


def plan_units():
    count = KVH // 2
    return [
        {
            "head": head,
            "far": 2 if head < LAG else 1,
            "told": 2 if head == count - 1 else 1,
            "later": head + LAG if head + LAG < count else None,
        }
        for head in range(count)
    ]


def on_pair(query_rows, key_rows, value_rows, out_grad, question_lengths):
    rows = query_rows.shape[0]
    group = QH // KVH
    low = jnp.bfloat16
    full = jnp.float32
    shape = jax.ShapeDtypeStruct
    units = plan_units()
    count = len(units)
    sib = [(0, 1), (1, 0), (2, 3), (3, 2)]
    same = [(0, 2), (1, 3), (2, 0), (3, 1)]
    cross = [(0, 3), (1, 2), (2, 1), (3, 0)]
    link = shape((rows, 2 * HD), low)
    wide = shape((rows, query_rows.shape[1] + key_rows.shape[1]), low)
    block = shape((group, 4 * rows, 2 * rows), low)

    def send(value, perm):
        return lax.ppermute(value, "sp", perm)

    place = lax.axis_index("sp").astype(jnp.int32).reshape(1)
    whole = (query_rows, out_grad, key_rows, value_rows, question_lengths)
    fixed = tuple(pltpu.with_memory_space_constraint(value, pltpu.HBM) for value in whole)
    *packs, sib_send = local_call(
        pack_kernel, [link] * (2 * LAG) + [wide], (place, *fixed[:4]), space=pltpu.HBM,
        scratch=[pltpu.SemaphoreType.DMA((4 * LAG + 4,))],
    )
    far = []
    for chunk in range(LAG):
        far.append((send(packs[2 * chunk], same), send(packs[2 * chunk + 1], cross)))
    sib_all = send(sib_send, sib)
    own_all, bias = local_call(
        stage_kernel, [wide, shape((2 * rows, 2 * rows), full)], (place, *fixed),
        space=pltpu.HBM,
        scratch=[
            pltpu.SMEM(question_lengths.shape, jnp.int32), pltpu.SemaphoreType.DMA((5,)),
        ],
    )
    wings = [shape((rows, group * HD), low)] * 2
    near = shape((rows, 2 * HD), full)
    dq_own, dq_sib, near_own, near_sib = [], [], [], []
    for index, unit in enumerate(units):
        split = unit["told"] == 2
        outs = local_call(
            partial(attend_kernel, unit),
            [*wings, near, near, link if split else shape((2 * rows, 2 * HD), low)]
            + ([block, block] if split else []),
            (place, bias, own_all, sib_all, *far[index]),
            flops=group * 10 * HD * 2 * rows * 4 * rows,
        )
        told = send(outs[4], same)
        if split:
            outs = local_call(
                partial(settle_kernel, unit),
                [wings[0], shape((rows, (group + 2) * HD), low), near, link],
                (place, own_all, sib_all, *far[index], *outs[:4], *outs[5:]),
                flops=group * 4 * HD * 2 * rows * 4 * rows,
            )
            told_cross = send(outs[3], cross)
            back_last = send(outs[1], sib)
            dq_last, near_last, told_last = outs[0], outs[2], told
        else:
            far.append((told,))
            dq_own.append(outs[0])
            dq_sib.append(send(outs[1], sib))
            near_own.append(outs[2])
            near_sib.append(outs[3])
    heard = [value[0] for value in far[LAG:]]
    back_keys, = local_call(
        partial(fold_kernel, count - 1), [shape((rows, (count - 1) * 2 * HD), low)],
        (place, *near_sib, *heard),
    )
    back_keys = send(back_keys, sib)
    shapes = [shape(value.shape, low) for value in (query_rows, key_rows, value_rows)]

    def join(part, args, results):
        spaces = [pltpu.VMEM] * len(args) + [pltpu.HBM] * len(results)
        return local_call(
            partial(join_kernel, part), shapes, (place, *args, *results),
            aliases={1 + len(args) + i: i for i in range(len(results))},
            in_spaces=spaces, out_space=pltpu.HBM,
            scratch=[
                pltpu.VMEM((len(part) + 1, rows, 2 * HD), low),
                pltpu.SemaphoreType.DMA((6 * len(part),)),
            ],
        )

    results = join(units[:-1], (*dq_own, *dq_sib, *near_own, *heard, back_keys), ())
    results = join(
        units[-1:], (dq_last, back_last, near_last, told_last, back_last, told_cross),
        results,
    )
    return tuple(results)


def solution(mesh):
    paired = mesh.shape["sp"] == 4
    rows = P(("grp", "sp"), None)
    return jax.shard_map(
        on_pair if paired else on_device,
        mesh=mesh,
        in_specs=(rows, rows, rows, rows, P("grp")),
        out_specs=(rows, rows, rows),
        check_vma=False,
    )
```

```python
from functools import partial
from functools import reduce
import math

import jax
import jax.numpy as jnp
from jax import lax
from jax.experimental import pallas as pl
from jax.experimental.pallas import tpu as pltpu
from jax.sharding import PartitionSpec as P

HD = 128
QH = 32
KVH = 8

LAG = 3
FOLDS = (2, 1)
STAGGER = [(stage, slot) for stage in range(3) for slot in range(4)]
STRIP = 64
VMEM_BYTES = 32 * 1024 * 1024


MASKED = -1e30


def widen(rows, copies):
    tokens = rows.shape[0]
    shaped = rows.reshape(tokens, KVH, 1, HD)
    return jnp.broadcast_to(shaped, (tokens, KVH, copies, HD)).reshape(tokens, KVH * copies * HD)


def segment_ids(question_lengths, length, doc_len):
    ends = jnp.cumsum(question_lengths)
    places = jnp.arange(length, dtype=jnp.int32)
    inside = jnp.sum((ends[None, :] <= (places - doc_len)[:, None]).astype(jnp.int32), axis=1)
    return jnp.where(places < doc_len, -1, inside)


def make_scores(query_block, key_block, visible, scaling):
    raw = (
        jnp.einsum("bkgd,skd->kgbs", query_block, key_block, preferred_element_type=jnp.float32)
        * scaling
    )
    return jnp.where(visible[None, None], raw, MASKED)


def weighted_values(probs_b, value_block):
    return jnp.einsum("kgbs,skd->bkgd", probs_b, value_block, preferred_element_type=jnp.float32)


def backward_block(probs, probs_b, delta, grad_block, query_block, key_block, value_block, scaling):
    value_part = jnp.einsum(
        "kgbs,bkgd->skd", probs_b, grad_block, preferred_element_type=jnp.float32
    )
    prob_grad = jnp.einsum(
        "bkgd,skd->kgbs", grad_block, value_block, preferred_element_type=jnp.float32
    )
    score_grad = (probs * (prob_grad - delta[..., None])).astype(jnp.bfloat16)
    query_part = jnp.einsum(
        "kgbs,skd->bkgd", score_grad, key_block, preferred_element_type=jnp.float32
    )
    key_part = (
        jnp.einsum("kgbs,bkgd->skd", score_grad, query_block, preferred_element_type=jnp.float32)
        * scaling
    )
    return (query_part, key_part, value_part)


def on_device(query_rows, key_rows, value_rows, out_grad, question_lengths):
    devices = lax.axis_size("sp")
    tokens = query_rows.shape[0]
    length = tokens * devices
    doc_len = length // 2
    block_len = min(512, length)
    block_count = length // block_len
    scaling = 1.0 / math.sqrt(HD)
    copies = max(KVH, devices) // KVH
    keys_local, values_local = (
        lax.all_to_all(widen(key_rows, copies), "sp", split_axis=1, concat_axis=0, tiled=True),
        lax.all_to_all(widen(value_rows, copies), "sp", split_axis=1, concat_axis=0, tiled=True),
    )
    queries_local, grads_local = (
        lax.all_to_all(query_rows, "sp", split_axis=1, concat_axis=0, tiled=True),
        lax.all_to_all(out_grad, "sp", split_axis=1, concat_axis=0, tiled=True),
    )
    key_heads = KVH * copies // devices
    per_group = QH // devices // key_heads
    queries = queries_local.reshape(length, key_heads, per_group, HD)
    grads = grads_local.reshape(length, key_heads, per_group, HD)
    keys = keys_local.reshape(length, key_heads, HD)
    values = values_local.reshape(length, key_heads, HD)
    segment = segment_ids(question_lengths, length, doc_len)
    places = jnp.arange(length, dtype=jnp.int32)
    query_shape = (block_len, key_heads, per_group, HD)
    key_shape = (block_len, key_heads, HD)
    key_sums = [jnp.zeros(key_shape, jnp.float32)] * block_count
    value_sums = [jnp.zeros(key_shape, jnp.float32)] * block_count
    query_parts = []
    for row_block in range(block_count):
        row_start = row_block * block_len
        query_block = queries[row_start : row_start + block_len]
        grad_block = grads[row_start : row_start + block_len]
        row_places = places[row_start : row_start + block_len]
        row_segment = segment[row_start : row_start + block_len]
        scores = []
        for col_block in range(row_block + 1):
            col_start = col_block * block_len
            col_places = places[col_start : col_start + block_len]
            col_segment = segment[col_start : col_start + block_len]
            visible = (col_places[None, :] <= row_places[:, None]) & (
                (col_places[None, :] < doc_len) | (col_segment[None, :] == row_segment[:, None])
            )
            scores.append(
                make_scores(query_block, keys[col_start : col_start + block_len], visible, scaling)
            )
        peak = reduce(jnp.maximum, [jnp.max(score, axis=3) for score in scores])
        total = reduce(
            jnp.add, [jnp.sum(jnp.exp(score - peak[..., None]), axis=3) for score in scores]
        )
        log_total = peak + jnp.log(total)
        probs = [jnp.exp(score - log_total[..., None]) for score in scores]
        probs_low = [single.astype(jnp.bfloat16) for single in probs]
        output = jnp.zeros(query_shape, jnp.float32)
        for col_block in range(row_block + 1):
            col_start = col_block * block_len
            output = output + weighted_values(
                probs_low[col_block], values[col_start : col_start + block_len]
            )
        output_low = output.astype(jnp.bfloat16)
        delta = jnp.einsum(
            "bkgd,bkgd->kgb", grad_block, output_low, preferred_element_type=jnp.float32
        )
        query_sum = jnp.zeros(query_shape, jnp.float32)
        for col_block in range(row_block + 1):
            col_start = col_block * block_len
            action = partial(
                backward_block,
                probs[col_block],
                probs_low[col_block],
                delta,
                grad_block,
                query_block,
                keys[col_start : col_start + block_len],
                values[col_start : col_start + block_len],
                scaling,
            )
            query_part, key_part, value_part = action()
            query_sum = query_sum + query_part
            key_sums[col_block] = key_sums[col_block] + key_part
            value_sums[col_block] = value_sums[col_block] + value_part
        query_parts.append((query_sum * scaling).astype(jnp.bfloat16))
    query_local = jnp.concatenate(query_parts, axis=0).reshape(length, key_heads * per_group * HD)
    key_local = jnp.concatenate(key_sums, axis=0).reshape(length, key_heads * HD)
    value_local = jnp.concatenate(value_sums, axis=0).reshape(length, key_heads * HD)
    query_grad = lax.all_to_all(query_local, "sp", split_axis=0, concat_axis=1, tiled=True)
    key_back, value_back = (
        lax.all_to_all(key_local, "sp", split_axis=0, concat_axis=1, tiled=True),
        lax.all_to_all(value_local, "sp", split_axis=0, concat_axis=1, tiled=True),
    )
    key_grad = (
        jnp.sum(key_back.reshape(tokens, KVH, copies, HD), axis=2)
        .reshape(tokens, KVH * HD)
        .astype(jnp.bfloat16)
    )
    value_grad = (
        jnp.sum(value_back.reshape(tokens, KVH, copies, HD), axis=2)
        .reshape(tokens, KVH * HD)
        .astype(jnp.bfloat16)
    )
    return (query_grad, key_grad, value_grad)


LOG2E = 1.4426950408889634
HIDDEN = -1e30


def contract(left, right, left_dim, right_dim):
    return lax.dot_general(
        left, right, (((left_dim,), (right_dim,)), ((), ())), preferred_element_type=jnp.float32
    )


def start_all(pairs, sems):
    copies = [pltpu.make_async_copy(src, dst, sems.at[i]) for i, (src, dst) in enumerate(pairs)]
    for copy in copies:
        copy.start()
    return copies


def halves_into(sources, side, out):
    pairs, at = [], 0
    for source in sources:
        half = source.shape[1] // 2
        start = pl.multiple_of(side * half, HD)
        pairs.append((source.at[:, pl.ds(start, half)], out.at[:, at : at + half]))
        at += half
    return pairs


def lend_pairs(core, sources, sib_send, own_first):
    pairs = halves_into(sources, 1 - core, sib_send)
    group = QH // KVH
    at = 0
    for source, width in zip(sources, (group * HD, group * HD, HD, HD)):
        start = pl.multiple_of(core * (source.shape[1] // 2), HD)
        pairs.append((source.at[:, pl.ds(start, width)], own_first.at[:, at : at + width]))
        at += width
    return pairs


def fill_bias(bias, spans, asking):
    spots = lax.broadcasted_iota(jnp.int32, bias.shape, 1)
    key_spots = lax.broadcasted_iota(jnp.int32, bias.shape, 0)
    visible = key_spots <= spots
    if asking:
        spot_row = lax.broadcasted_iota(jnp.int32, (1, bias.shape[1]), 1)
        begin = jnp.zeros((1, bias.shape[1]), jnp.int32)
        end = jnp.int32(0)
        for question in range(spans.shape[0]):
            end = end + spans[question]
            begin = begin + jnp.where(spot_row >= end, spans[question], 0)
        visible = visible & (key_spots >= begin)
    bias[...] = jnp.where(visible, 0.0, HIDDEN)


def pack_kernel(place, queries, grads, keys, values, *refs):
    *sends, sib_send, own_first, bias, sems = refs
    core = place[0] % 2
    half = keys.shape[1] // 2

    @pl.when(place[0] // 2 == 0)
    def _():
        pairs = []
        for index, out in enumerate(sends):
            chunk, side = index // 2, index % 2
            base = (core if side == 0 else 1 - core) * half
            start = pl.multiple_of(base + chunk * HD, HD)
            pairs.append((keys.at[:, pl.ds(start, HD)], out.at[:, :HD]))
            pairs.append((values.at[:, pl.ds(start, HD)], out.at[:, HD:]))
        pairs += lend_pairs(core, (queries, grads, keys, values), sib_send, own_first)
        copies = start_all(pairs, sems)
        fill_bias(bias, None, False)
        for copy in copies:
            copy.wait()


def lend_kernel(place, queries, grads, keys, values, lengths, *refs):
    sib_send, own_first, bias, spans, sems = refs[-5:]

    @pl.when(place[0] // 2 == 1)
    def _():
        sources = (queries, grads, keys, values)
        pairs = [(lengths, spans)] + lend_pairs(place[0] % 2, sources, sib_send, own_first)
        copies = start_all(pairs, sems)
        copies[0].wait()
        fill_bias(bias, spans, True)
        for copy in copies[1:]:
            copy.wait()


def specialise(place, body):
    core, asking = place[0] % 2, place[0] // 2
    for first in (True, False):
        for asks in (True, False):
            @pl.when((core == (0 if first else 1)) & (asking == (1 if asks else 0)))
            def _(first=first, asks=asks):
                body(asks, (lambda own, sib: (own, sib)) if first else (lambda own, sib: (sib, own)))


def columns(own_all, head):
    group = QH // KVH
    heads = own_all.shape[1] // (2 * (group + 1) * HD)
    query_at, grad_at = head * group * HD, (heads + head) * group * HD
    key_at = (2 * heads * group + head) * HD
    return query_at, grad_at, key_at, key_at + heads * HD


def head_columns(ref, head):
    group = QH // KVH
    if ref.shape[1] == KVH * (group + 1) * HD:
        return columns(ref, head)
    return 0, group * HD, 2 * group * HD, (2 * group + 1) * HD


def stacked(ref, at, pair):
    first = at + 2 * pair * HD
    return jnp.concatenate([ref[:, first : first + HD], ref[:, first + HD : first + 2 * HD]], axis=0)


def head_parts(asks, order, own, sib_all, far, head):
    near = order((own, *head_columns(own, head)), (sib_all, *head_columns(sib_all, head)))
    keys = [ref[:, at : at + HD] for ref, _, _, at, _ in near]
    values = [ref[:, at : at + HD] for ref, _, _, _, at in near]
    if asks:
        distant = order(*far) if len(far) == 2 else far
        keys = [ref[:, :HD] for ref in distant] + keys
        values = [ref[:, HD:] for ref in distant] + values
    queries = lambda side, pair: stacked(near[side][0], near[side][1], pair)
    grads = lambda side, pair: stacked(near[side][0], near[side][2], pair)
    return queries, grads, jnp.concatenate(keys, axis=0), jnp.concatenate(values, axis=0)


def fold_rows(op, value):
    return op(value.reshape(value.shape[0] // 8, 8, value.shape[1]), axis=0)


def score(keys, values, q, g, hide, distant):
    scores = contract(keys, q, 1, 1)
    hide = jnp.concatenate([hide, hide], axis=1)
    parts, peak = [], None
    for start in range(0, scores.shape[0], STRIP):
        part = scores[start : start + STRIP]
        if start >= distant:
            part = part + hide[start - distant : start - distant + STRIP]
        parts.append(part)
        top = fold_rows(jnp.max, part)
        peak = top if peak is None else jnp.maximum(peak, top)
    return parts, jnp.max(peak, axis=0, keepdims=True), contract(values, g, 1, 1)


def soften(parts, peak, prob_grad, power):
    exps, total, weighted = [], 0.0, 0.0
    grads = [prob_grad[i * STRIP : (i + 1) * STRIP] for i in range(len(parts))]
    for part, grad in zip(parts, grads):
        exp = jnp.exp2((part - peak) * power)
        exps.append(exp)
        total = total + fold_rows(jnp.sum, exp)
        weighted = weighted + fold_rows(jnp.sum, exp * grad)
    inverse = 1.0 / jnp.sum(total, axis=0, keepdims=True)
    delta = jnp.sum(weighted, axis=0, keepdims=True) * inverse
    probs, score_grads = [], []
    for exp, grad in zip(exps, grads):
        prob = exp * inverse
        probs.append(prob.astype(jnp.bfloat16))
        score_grads.append((prob * (grad - delta)).astype(jnp.bfloat16))
    return jnp.concatenate(probs, axis=0), jnp.concatenate(score_grads, axis=0)


def accumulate(sums, slot, value):
    sums[slot] = value if sums[slot] is None else sums[slot] + value


def attend_kernel(unit, place, bias, own_all, sib_all, *refs):
    refs = list(refs)
    far = [refs.pop(0) for _ in range(unit["far"])]
    split = unit["told"] == 2
    copies, own_rest = [], own_all
    if unit["head"] == 0:
        *refs, own_rest, sems = refs
        copies = start_all(halves_into(refs[:4], place[0] % 2, own_rest), sems)
    outs = refs[-5 if not split else -7 :]
    dq_own, dq_sib, near_own, near_sib, out = outs[:5]
    head = unit["head"]
    rows = own_all.shape[0]
    scaling = 1.0 / math.sqrt(HD)
    power = scaling * LOG2E
    low = jnp.bfloat16

    def pass_on(asks, order):
        if asks or unit["later"] is None:
            return
        _, _, later_key, later_value = columns(sib_all, unit["later"])
        for half, ref in enumerate(order(own_rest, sib_all)):
            spot = slice(half * rows, (half + 1) * rows)
            out[spot, :HD] = ref[:, later_key : later_key + HD]
            out[spot, HD:] = ref[:, later_value : later_value + HD]

    def body(asks, order):
        if not copies:
            pass_on(asks, order)
        distant = 2 * rows if asks else 0
        queries, grads, keys, values = head_parts(asks, order, own_all, sib_all, far, head)
        partial_only = split and asks
        keys_t = None if partial_only else keys.T
        dk, dv, told = [None, None], [None, None], [None, None]
        held = {}

        def first_stage(slot):
            pair, side = slot // 2, slot % 2
            q, g = queries(side, pair), grads(side, pair)
            count = distant + (side + 1) * rows
            hide = bias[: (side + 1) * rows, side * rows : (side + 1) * rows]
            held[slot] = (q, g, *score(keys[:count], values[:count], q, g, hide, distant))

        def second_stage(slot):
            q, g, scores, peak, prob_grad = held[slot]
            held[slot] = (q, g, *soften(scores, peak, prob_grad, power))

        def third_stage(slot):
            pair, side = slot // 2, slot % 2
            count = distant + (side + 1) * rows
            q, g, probs, score_grad = held.pop(slot)
            if partial_only:
                outs[5][slot, :count] = probs
                outs[6][slot, :count] = score_grad
                wanted = order(0, rows)[0]
                accumulate(told, 0, contract(score_grad[wanted : wanted + rows], q, 1, 0))
                accumulate(told, 1, contract(probs[wanted : wanted + rows], g, 1, 0))
                return
            accumulate(dv, side, contract(probs, g, 1, 0))
            accumulate(dk, side, contract(score_grad, q, 1, 0))
            dq = (contract(keys_t[:, :count], score_grad, 1, 0) * scaling).T.astype(low)
            target = order(dq_own, dq_sib)[side]
            for member in range(2):
                at = (pair * 2 + member) * HD
                target[:, at : at + HD] = dq[member * rows : (member + 1) * rows]

        stages = (first_stage, second_stage, third_stage)
        for stage, slot in STAGGER:
            stages[stage](slot)
        if partial_only:
            out[:, :HD] = (told[0] * scaling).astype(low)
            out[:, HD:] = told[1].astype(low)
            return
        for slot, (lo, hi) in enumerate((dk, dv)):
            size = scaling if slot == 0 else 1.0
            spot = slice(slot * HD, (slot + 1) * HD)
            first, second = order(near_own, near_sib)
            first[:, spot] = (lo[distant:] + hi[distant : distant + rows]) * size
            second[:, spot] = hi[distant + rows :] * size
            if asks:
                out[:, spot] = ((lo[:distant] + hi[:distant]) * size).astype(low)

    specialise(place, body)
    if copies:
        for copy in copies:
            copy.wait()
        specialise(place, pass_on)


def settle_kernel(unit, place, own_all, sib_all, *refs):
    refs = list(refs)
    far = [refs.pop(0) for _ in range(unit["far"])]
    dq_own_in, dq_sib_in, near_own_in, near_sib_in, probs_in, grads_in = refs[:6]
    dq_own, back, near_own, out = refs[6:]
    rows = own_all.shape[0]
    group = QH // KVH
    scaling = 1.0 / math.sqrt(HD)
    low = jnp.bfloat16

    def body(asks, order):
        if not asks:
            dq_own[...] = dq_own_in[...]
            near_own[...] = near_own_in[...]
            back[:, : group * HD] = dq_sib_in[...]
            back[:, group * HD :] = near_sib_in[...].astype(low)
            return
        queries, grads, keys, _ = head_parts(asks, order, own_all, sib_all, far, unit["head"])
        keys_t = keys.T
        distant = 2 * rows
        dk, dv, told = [None, None], [None, None], [None, None]
        for pair in range(group // 2):
            for side in range(2):
                slot = pair * 2 + side
                count = distant + (side + 1) * rows
                q, g = queries(side, pair), grads(side, pair)
                probs, score_grad = probs_in[slot, :count], grads_in[slot, :count]
                wanted = order(0, rows)[1]
                accumulate(told, 0, contract(score_grad[wanted : wanted + rows], q, 1, 0))
                accumulate(told, 1, contract(probs[wanted : wanted + rows], g, 1, 0))
                accumulate(dv, side, contract(probs[distant:], g, 1, 0))
                accumulate(dk, side, contract(score_grad[distant:], q, 1, 0))
                dq = (contract(keys_t[:, :count], score_grad, 1, 0) * scaling).T.astype(low)
                target = order(dq_own, back)[side]
                for member in range(2):
                    at = (pair * 2 + member) * HD
                    target[:, at : at + HD] = dq[member * rows : (member + 1) * rows]
        for slot, (lo, hi) in enumerate((dk, dv)):
            size = scaling if slot == 0 else 1.0
            at = slot * HD
            targets = order((near_own, at), (back, group * HD + at))
            for (target, spot), value in zip(targets, (lo + hi[:rows], hi[rows:])):
                target[:, spot : spot + HD] = (value * size).astype(target.dtype)
            out[:, at : at + HD] = (told[slot] * size).astype(low)

    specialise(place, body)


def fold_kernel(count, place, *refs):
    nears, tolds, back = refs[:count], refs[count : 2 * count], refs[-1]
    core = place[0] % 2
    hears = place[0] // 2 == 0
    rows, width = nears[0].shape
    at = pl.multiple_of((1 - core) * rows, rows)
    for index in range(count):
        told = jnp.where(hears, tolds[index][pl.ds(at, rows), :].astype(jnp.float32), 0.0)
        back[:, index * width : (index + 1) * width] = (nears[index][...] + told).astype(back.dtype)


def join_kernel(plan, place, *refs):
    outs, (sums, sems) = refs[-5:-2], refs[-2:]
    core = place[0] % 2
    hears = place[0] // 2 == 0
    group = QH // KVH
    halves = [out.shape[1] // 2 for out in outs]
    rows = sums.shape[1]
    own_rows = pl.multiple_of(core * rows, HD)
    copies = []

    def write(source, out, start, width):
        target = out.at[:, pl.ds(pl.multiple_of(start, HD), width)]
        copies.append(pltpu.make_async_copy(source, target, sems.at[len(copies)]))
        copies[-1].start()

    def write_pair(source, at, head, owner):
        for slot in range(2):
            spot = slice(at + slot * HD, at + (slot + 1) * HD)
            write(source.at[:, spot], outs[1 + slot], owner * halves[1] + head * HD, HD)

    for head, own, other in plan["queries"]:
        width = group * HD
        write(refs[own], outs[0], core * halves[0] + head * width, width)
        write(refs[other].at[:, :width], outs[0], (1 - core) * halves[0] + head * width, width)
    for head, other, at in plan["ready"]:
        write_pair(refs[other], at, head, 1 - core)
    cell = 0
    for head, near, told, direct in plan["own"]:
        heard = refs[told][...] if direct else refs[told][pl.ds(own_rows, rows), :]
        total = refs[near][...] + jnp.where(hears, heard.astype(jnp.float32), 0.0)
        sums[cell] = total.astype(sums.dtype)
        write_pair(sums.at[cell], 0, head, core)
        cell += 1
    for head, other, at, told in plan["other"]:
        total = refs[other][:, at : at + 2 * HD].astype(jnp.float32)
        total = total + jnp.where(hears, refs[told][...].astype(jnp.float32), 0.0)
        sums[cell] = total.astype(sums.dtype)
        write_pair(sums.at[cell], 0, head, 1 - core)
        cell += 1
    for copy in copies:
        copy.wait()


def local_call(kernel, outs, args, scratch=(), flops=0, space=pltpu.VMEM, aliases=None, out_space=pltpu.VMEM, in_spaces=None):
    specs = [pl.BlockSpec(memory_space=pltpu.SMEM)]
    specs += [pl.BlockSpec(memory_space=kind) for kind in in_spaces or [space] * (len(args) - 1)]
    return pl.pallas_call(
        kernel,
        out_shape=tuple(outs),
        in_specs=specs,
        out_specs=tuple(pl.BlockSpec(memory_space=out_space) for _ in outs),
        scratch_shapes=scratch,
        input_output_aliases=aliases or {},
        compiler_params=pltpu.CompilerParams(vmem_limit_bytes=VMEM_BYTES),
        cost_estimate=pl.CostEstimate(flops=flops, transcendentals=0, bytes_accessed=0),
    )(*args)


def plan_units():
    count = KVH // 2
    return [
        {
            "head": head,
            "far": 2 if head < LAG else 1,
            "told": 2 if head == count - 1 else 1,
            "later": head + LAG if head + LAG < count else None,
        }
        for head in range(count)
    ]


def on_pair(query_rows, key_rows, value_rows, out_grad, question_lengths):
    rows = query_rows.shape[0]
    group = QH // KVH
    low = jnp.bfloat16
    full = jnp.float32
    shape = jax.ShapeDtypeStruct
    units = plan_units()
    count = len(units)
    sib = [(0, 1), (1, 0), (2, 3), (3, 2)]
    same = [(0, 2), (1, 3), (2, 0), (3, 1)]
    cross = [(0, 3), (1, 2), (2, 1), (3, 0)]
    link = shape((rows, 2 * HD), low)
    wide = shape((rows, query_rows.shape[1] + key_rows.shape[1]), low)
    block = shape((group, 4 * rows, 2 * rows), low)

    def send(value, perm):
        return lax.ppermute(value, "sp", perm)

    place = lax.axis_index("sp").astype(jnp.int32).reshape(1)
    whole = (query_rows, out_grad, key_rows, value_rows, question_lengths)
    fixed = tuple(pltpu.with_memory_space_constraint(value, pltpu.HBM) for value in whole)
    narrow = shape((rows, 2 * (group + 1) * HD), low)
    lent = [wide, narrow, shape((2 * rows, 2 * rows), full)]
    *packs, sib_send, own_first, bias = local_call(
        pack_kernel, [link] * (2 * LAG) + lent, (place, *fixed[:4]), space=pltpu.HBM,
        scratch=[pltpu.SemaphoreType.DMA((4 * LAG + 8,))],
    )
    args = (place, *fixed, sib_send, own_first, bias)
    sib_send, own_first, bias = local_call(
        lend_kernel, lent, args, aliases={6 + i: i for i in range(3)},
        in_spaces=[pltpu.HBM] * 5 + [pltpu.VMEM] * 3,
        scratch=[
            pltpu.SMEM(question_lengths.shape, jnp.int32), pltpu.SemaphoreType.DMA((9,)),
        ],
    )
    far = []
    for chunk in range(LAG):
        far.append((send(packs[2 * chunk], same), send(packs[2 * chunk + 1], cross)))
    sib_all = send(sib_send, sib)
    wings = [shape((rows, group * HD), low)] * 2
    near = shape((rows, 2 * HD), full)
    dq_own, dq_sib, near_own, near_sib = [], [], [], []
    for index, unit in enumerate(units):
        split = unit["told"] == 2
        lead = index == 0
        args = (place, bias, own_first if lead else own_all, sib_all, *far[index])
        outs = local_call(
            partial(attend_kernel, unit),
            [*wings, near, near, link if split else shape((2 * rows, 2 * HD), low)]
            + ([block, block] if split else []) + ([wide] if lead else []),
            args + (fixed[:4] if lead else ()),
            in_spaces=[pltpu.VMEM] * (len(args) - 1) + [pltpu.HBM] * (4 if lead else 0),
            scratch=[pltpu.SemaphoreType.DMA((4,))] if lead else (),
            flops=group * 10 * HD * 2 * rows * 4 * rows,
        )
        if lead:
            own_all = outs[5]
        told = send(outs[4], same)
        if split:
            outs = local_call(
                partial(settle_kernel, unit),
                [wings[0], shape((rows, (group + 2) * HD), low), near, link],
                (place, own_all, sib_all, *far[index], *outs[:4], *outs[5:]),
                flops=group * 4 * HD * 2 * rows * 4 * rows,
            )
            told_cross = send(outs[3], cross)
            back_last = send(outs[1], sib)
            dq_last, near_last, told_last = outs[0], outs[2], told
        else:
            far.append((told,))
            dq_own.append(outs[0])
            dq_sib.append(send(outs[1], sib))
            near_own.append(outs[2])
            near_sib.append(outs[3])
    heard = [value[0] for value in far[LAG:]]
    shapes = [shape(value.shape, low) for value in (query_rows, key_rows, value_rows)]
    ready, head = [], 0
    for size in FOLDS:
        span = slice(head, head + size)
        folded, = local_call(
            partial(fold_kernel, size), [shape((rows, size * 2 * HD), low)],
            (place, *near_sib[span], *heard[span]),
        )
        folded = send(folded, sib)
        ready.append([(head + i, folded, 2 * i * HD) for i in range(size)])
        head += size

    def join(results, queries, own, ready, other):
        args = []

        def use(value):
            args.append(value)
            return len(args) - 1

        plan = {
            "queries": [(at, use(first), use(second)) for at, first, second in queries],
            "ready": [(at, use(value), spot) for at, value, spot in ready],
            "own": [(at, use(near), use(told), direct) for at, near, told, direct in own],
            "other": [(at, use(value), spot, use(told)) for at, value, spot, told in other],
        }
        cells = len(own) + len(other)
        writes = 2 * (len(queries) + len(ready) + cells)
        return local_call(
            partial(join_kernel, plan), shapes, (place, *args, *results),
            aliases={1 + len(args) + i: i for i in range(len(results))},
            in_spaces=[pltpu.VMEM] * len(args) + [pltpu.HBM] * len(results),
            out_space=pltpu.HBM,
            scratch=[pltpu.VMEM((cells, rows, 2 * HD), low), pltpu.SemaphoreType.DMA((writes,))],
        )

    last = count - 1
    queries = [(i, dq_own[i], dq_sib[i]) for i in range(last)]
    own = [(i, near_own[i], heard[i], False) for i in range(last)]
    soon = sum(FOLDS[:-1])
    results = join((), queries, own[:soon], [item for part in ready[:-1] for item in part], ())
    results = join(
        results, [(last, dq_last, back_last)],
        own[soon:] + [(last, near_last, told_last, True)], ready[-1],
        [(last, back_last, group * HD, told_cross)],
    )
    return tuple(results)


def solution(mesh):
    paired = mesh.shape["sp"] == 4
    rows = P(("grp", "sp"), None)
    return jax.shard_map(
        on_pair if paired else on_device,
        mesh=mesh,
        in_specs=(rows, rows, rows, rows, P("grp")),
        out_specs=(rows, rows, rows),
        check_vma=False,
    )
```

```python
from functools import partial
from functools import reduce
import math

import jax
import jax.numpy as jnp
from jax import lax
from jax.experimental import pallas as pl
from jax.experimental.pallas import tpu as pltpu
from jax.sharding import PartitionSpec as P

HD = 128
QH = 32
KVH = 8

LAG = 3
FOLDS = (2, 1)
STAGGER = [(stage, slot) for stage in range(3) for slot in range(4)]
STRIP = 64
VMEM_BYTES = 32 * 1024 * 1024


MASKED = -1e30


def widen(rows, copies):
    tokens = rows.shape[0]
    shaped = rows.reshape(tokens, KVH, 1, HD)
    return jnp.broadcast_to(shaped, (tokens, KVH, copies, HD)).reshape(tokens, KVH * copies * HD)


def segment_ids(question_lengths, length, doc_len):
    ends = jnp.cumsum(question_lengths)
    places = jnp.arange(length, dtype=jnp.int32)
    inside = jnp.sum((ends[None, :] <= (places - doc_len)[:, None]).astype(jnp.int32), axis=1)
    return jnp.where(places < doc_len, -1, inside)


def make_scores(query_block, key_block, visible, scaling):
    raw = (
        jnp.einsum("bkgd,skd->kgbs", query_block, key_block, preferred_element_type=jnp.float32)
        * scaling
    )
    return jnp.where(visible[None, None], raw, MASKED)


def weighted_values(probs_b, value_block):
    return jnp.einsum("kgbs,skd->bkgd", probs_b, value_block, preferred_element_type=jnp.float32)


def backward_block(probs, probs_b, delta, grad_block, query_block, key_block, value_block, scaling):
    value_part = jnp.einsum(
        "kgbs,bkgd->skd", probs_b, grad_block, preferred_element_type=jnp.float32
    )
    prob_grad = jnp.einsum(
        "bkgd,skd->kgbs", grad_block, value_block, preferred_element_type=jnp.float32
    )
    score_grad = (probs * (prob_grad - delta[..., None])).astype(jnp.bfloat16)
    query_part = jnp.einsum(
        "kgbs,skd->bkgd", score_grad, key_block, preferred_element_type=jnp.float32
    )
    key_part = (
        jnp.einsum("kgbs,bkgd->skd", score_grad, query_block, preferred_element_type=jnp.float32)
        * scaling
    )
    return (query_part, key_part, value_part)


def on_device(query_rows, key_rows, value_rows, out_grad, question_lengths):
    devices = lax.axis_size("sp")
    tokens = query_rows.shape[0]
    length = tokens * devices
    doc_len = length // 2
    block_len = min(512, length)
    block_count = length // block_len
    scaling = 1.0 / math.sqrt(HD)
    copies = max(KVH, devices) // KVH
    keys_local, values_local = (
        lax.all_to_all(widen(key_rows, copies), "sp", split_axis=1, concat_axis=0, tiled=True),
        lax.all_to_all(widen(value_rows, copies), "sp", split_axis=1, concat_axis=0, tiled=True),
    )
    queries_local, grads_local = (
        lax.all_to_all(query_rows, "sp", split_axis=1, concat_axis=0, tiled=True),
        lax.all_to_all(out_grad, "sp", split_axis=1, concat_axis=0, tiled=True),
    )
    key_heads = KVH * copies // devices
    per_group = QH // devices // key_heads
    queries = queries_local.reshape(length, key_heads, per_group, HD)
    grads = grads_local.reshape(length, key_heads, per_group, HD)
    keys = keys_local.reshape(length, key_heads, HD)
    values = values_local.reshape(length, key_heads, HD)
    segment = segment_ids(question_lengths, length, doc_len)
    places = jnp.arange(length, dtype=jnp.int32)
    query_shape = (block_len, key_heads, per_group, HD)
    key_shape = (block_len, key_heads, HD)
    key_sums = [jnp.zeros(key_shape, jnp.float32)] * block_count
    value_sums = [jnp.zeros(key_shape, jnp.float32)] * block_count
    query_parts = []
    for row_block in range(block_count):
        row_start = row_block * block_len
        query_block = queries[row_start : row_start + block_len]
        grad_block = grads[row_start : row_start + block_len]
        row_places = places[row_start : row_start + block_len]
        row_segment = segment[row_start : row_start + block_len]
        scores = []
        for col_block in range(row_block + 1):
            col_start = col_block * block_len
            col_places = places[col_start : col_start + block_len]
            col_segment = segment[col_start : col_start + block_len]
            visible = (col_places[None, :] <= row_places[:, None]) & (
                (col_places[None, :] < doc_len) | (col_segment[None, :] == row_segment[:, None])
            )
            scores.append(
                make_scores(query_block, keys[col_start : col_start + block_len], visible, scaling)
            )
        peak = reduce(jnp.maximum, [jnp.max(score, axis=3) for score in scores])
        total = reduce(
            jnp.add, [jnp.sum(jnp.exp(score - peak[..., None]), axis=3) for score in scores]
        )
        log_total = peak + jnp.log(total)
        probs = [jnp.exp(score - log_total[..., None]) for score in scores]
        probs_low = [single.astype(jnp.bfloat16) for single in probs]
        output = jnp.zeros(query_shape, jnp.float32)
        for col_block in range(row_block + 1):
            col_start = col_block * block_len
            output = output + weighted_values(
                probs_low[col_block], values[col_start : col_start + block_len]
            )
        output_low = output.astype(jnp.bfloat16)
        delta = jnp.einsum(
            "bkgd,bkgd->kgb", grad_block, output_low, preferred_element_type=jnp.float32
        )
        query_sum = jnp.zeros(query_shape, jnp.float32)
        for col_block in range(row_block + 1):
            col_start = col_block * block_len
            action = partial(
                backward_block,
                probs[col_block],
                probs_low[col_block],
                delta,
                grad_block,
                query_block,
                keys[col_start : col_start + block_len],
                values[col_start : col_start + block_len],
                scaling,
            )
            query_part, key_part, value_part = action()
            query_sum = query_sum + query_part
            key_sums[col_block] = key_sums[col_block] + key_part
            value_sums[col_block] = value_sums[col_block] + value_part
        query_parts.append((query_sum * scaling).astype(jnp.bfloat16))
    query_local = jnp.concatenate(query_parts, axis=0).reshape(length, key_heads * per_group * HD)
    key_local = jnp.concatenate(key_sums, axis=0).reshape(length, key_heads * HD)
    value_local = jnp.concatenate(value_sums, axis=0).reshape(length, key_heads * HD)
    query_grad = lax.all_to_all(query_local, "sp", split_axis=0, concat_axis=1, tiled=True)
    key_back, value_back = (
        lax.all_to_all(key_local, "sp", split_axis=0, concat_axis=1, tiled=True),
        lax.all_to_all(value_local, "sp", split_axis=0, concat_axis=1, tiled=True),
    )
    key_grad = (
        jnp.sum(key_back.reshape(tokens, KVH, copies, HD), axis=2)
        .reshape(tokens, KVH * HD)
        .astype(jnp.bfloat16)
    )
    value_grad = (
        jnp.sum(value_back.reshape(tokens, KVH, copies, HD), axis=2)
        .reshape(tokens, KVH * HD)
        .astype(jnp.bfloat16)
    )
    return (query_grad, key_grad, value_grad)


LOG2E = 1.4426950408889634
HIDDEN = -1e30


def contract(left, right, left_dim, right_dim):
    return lax.dot_general(
        left, right, (((left_dim,), (right_dim,)), ((), ())), preferred_element_type=jnp.float32
    )


def start_all(pairs, sems):
    copies = [pltpu.make_async_copy(src, dst, sems.at[i]) for i, (src, dst) in enumerate(pairs)]
    for copy in copies:
        copy.start()
    return copies


def halves_into(sources, side, out):
    pairs, at = [], 0
    for source in sources:
        half = source.shape[1] // 2
        start = pl.multiple_of(side * half, HD)
        pairs.append((source.at[:, pl.ds(start, half)], out.at[:, at : at + half]))
        at += half
    return pairs


def lend_pairs(core, sources, sib_send, own_first):
    pairs = halves_into(sources, 1 - core, sib_send)
    group = QH // KVH
    at = 0
    for source, width in zip(sources, (group * HD, group * HD, HD, HD)):
        start = pl.multiple_of(core * (source.shape[1] // 2), HD)
        pairs.append((source.at[:, pl.ds(start, width)], own_first.at[:, at : at + width]))
        at += width
    return pairs


def fill_bias(bias, spans, asking):
    spots = lax.broadcasted_iota(jnp.int32, bias.shape, 1)
    key_spots = lax.broadcasted_iota(jnp.int32, bias.shape, 0)
    visible = key_spots <= spots
    if asking:
        spot_row = lax.broadcasted_iota(jnp.int32, (1, bias.shape[1]), 1)
        begin = jnp.zeros((1, bias.shape[1]), jnp.int32)
        end = jnp.int32(0)
        for question in range(spans.shape[0]):
            end = end + spans[question]
            begin = begin + jnp.where(spot_row >= end, spans[question], 0)
        visible = visible & (key_spots >= begin)
    bias[...] = jnp.where(visible, 0.0, HIDDEN)


def pack_kernel(place, queries, grads, keys, values, *refs):
    *sends, sib_send, own_first, bias, sems = refs
    core = place[0] % 2
    half = keys.shape[1] // 2

    @pl.when(place[0] // 2 == 0)
    def _():
        pairs = []
        for index, out in enumerate(sends):
            chunk, side = index // 2, index % 2
            base = (core if side == 0 else 1 - core) * half
            start = pl.multiple_of(base + chunk * HD, HD)
            pairs.append((keys.at[:, pl.ds(start, HD)], out.at[:, :HD]))
            pairs.append((values.at[:, pl.ds(start, HD)], out.at[:, HD:]))
        pairs += lend_pairs(core, (queries, grads, keys, values), sib_send, own_first)
        copies = start_all(pairs, sems)
        fill_bias(bias, None, False)
        for copy in copies:
            copy.wait()


def lend_kernel(place, queries, grads, keys, values, lengths, *refs):
    sib_send, own_first, bias, spans, sems = refs[-5:]

    @pl.when(place[0] // 2 == 1)
    def _():
        sources = (queries, grads, keys, values)
        pairs = [(lengths, spans)] + lend_pairs(place[0] % 2, sources, sib_send, own_first)
        copies = start_all(pairs, sems)
        copies[0].wait()
        fill_bias(bias, spans, True)
        for copy in copies[1:]:
            copy.wait()


def specialise(place, body):
    core, asking = place[0] % 2, place[0] // 2
    for first in (True, False):
        for asks in (True, False):
            @pl.when((core == (0 if first else 1)) & (asking == (1 if asks else 0)))
            def _(first=first, asks=asks):
                body(asks, (lambda own, sib: (own, sib)) if first else (lambda own, sib: (sib, own)))


def columns(own_all, head):
    group = QH // KVH
    heads = own_all.shape[1] // (2 * (group + 1) * HD)
    query_at, grad_at = head * group * HD, (heads + head) * group * HD
    key_at = (2 * heads * group + head) * HD
    return query_at, grad_at, key_at, key_at + heads * HD


def head_columns(ref, head):
    group = QH // KVH
    if ref.shape[1] == KVH * (group + 1) * HD:
        return columns(ref, head)
    return 0, group * HD, 2 * group * HD, (2 * group + 1) * HD


def stacked(ref, at, pair):
    first = at + 2 * pair * HD
    return jnp.concatenate([ref[:, first : first + HD], ref[:, first + HD : first + 2 * HD]], axis=0)


def head_parts(asks, order, own, sib_all, far, head):
    near = order((own, *head_columns(own, head)), (sib_all, *head_columns(sib_all, head)))
    keys = [ref[:, at : at + HD] for ref, _, _, at, _ in near]
    values = [ref[:, at : at + HD] for ref, _, _, _, at in near]
    if asks:
        distant = order(*far) if len(far) == 2 else far
        keys = [ref[:, :HD] for ref in distant] + keys
        values = [ref[:, HD:] for ref in distant] + values
    queries = lambda side, pair: stacked(near[side][0], near[side][1], pair)
    grads = lambda side, pair: stacked(near[side][0], near[side][2], pair)
    return queries, grads, jnp.concatenate(keys, axis=0), jnp.concatenate(values, axis=0)


def fold_rows(op, value):
    return op(value.reshape(value.shape[0] // 8, 8, value.shape[1]), axis=0)


def score(keys, values, q, g, hide, distant):
    scores = contract(keys, q, 1, 1)
    hide = jnp.concatenate([hide, hide], axis=1)
    parts, peak = [], None
    for start in range(0, scores.shape[0], STRIP):
        part = scores[start : start + STRIP]
        if start >= distant:
            part = part + hide[start - distant : start - distant + STRIP]
        parts.append(part)
        top = fold_rows(jnp.max, part)
        peak = top if peak is None else jnp.maximum(peak, top)
    return parts, jnp.max(peak, axis=0, keepdims=True), contract(values, g, 1, 1)


def soften(parts, peak, prob_grad, power):
    exps, total, weighted = [], 0.0, 0.0
    grads = [prob_grad[i * STRIP : (i + 1) * STRIP] for i in range(len(parts))]
    for part, grad in zip(parts, grads):
        exp = jnp.exp2((part - peak) * power)
        exps.append(exp)
        total = total + fold_rows(jnp.sum, exp)
        weighted = weighted + fold_rows(jnp.sum, exp * grad)
    inverse = 1.0 / jnp.sum(total, axis=0, keepdims=True)
    delta = jnp.sum(weighted, axis=0, keepdims=True) * inverse
    probs, score_grads = [], []
    for exp, grad in zip(exps, grads):
        prob = exp * inverse
        probs.append(prob.astype(jnp.bfloat16))
        score_grads.append((prob * (grad - delta)).astype(jnp.bfloat16))
    return jnp.concatenate(probs, axis=0), jnp.concatenate(score_grads, axis=0)


def accumulate(sums, slot, value):
    sums[slot] = value if sums[slot] is None else sums[slot] + value


def attend_kernel(unit, place, bias, own_all, sib_all, *refs):
    refs = list(refs)
    far = [refs.pop(0) for _ in range(unit["far"])]
    split = unit["told"] == 2
    copies, own_rest = [], own_all
    if unit["head"] == 0:
        *refs, own_rest, sems = refs
        copies = start_all(halves_into(refs[:4], place[0] % 2, own_rest), sems)
    outs = refs[-5 if not split else -7 :]
    dq_own, dq_sib, near_own, near_sib, out = outs[:5]
    head = unit["head"]
    rows = own_all.shape[0]
    scaling = 1.0 / math.sqrt(HD)
    power = scaling * LOG2E
    low = jnp.bfloat16

    def pass_on(asks, order):
        if asks or unit["later"] is None:
            return
        _, _, later_key, later_value = columns(sib_all, unit["later"])
        for half, ref in enumerate(order(own_rest, sib_all)):
            spot = slice(half * rows, (half + 1) * rows)
            out[spot, :HD] = ref[:, later_key : later_key + HD]
            out[spot, HD:] = ref[:, later_value : later_value + HD]

    def body(asks, order):
        if not copies:
            pass_on(asks, order)
        distant = 2 * rows if asks else 0
        queries, grads, keys, values = head_parts(asks, order, own_all, sib_all, far, head)
        partial_only = split and asks
        keys_t = None if partial_only else keys.T
        dk, dv, told = [None, None], [None, None], [None, None]
        held = {}

        def first_stage(slot):
            pair, side = slot // 2, slot % 2
            q, g = queries(side, pair), grads(side, pair)
            count = distant + (side + 1) * rows
            hide = bias[: (side + 1) * rows, side * rows : (side + 1) * rows]
            held[slot] = (q, g, *score(keys[:count], values[:count], q, g, hide, distant))

        def second_stage(slot):
            q, g, scores, peak, prob_grad = held[slot]
            held[slot] = (q, g, *soften(scores, peak, prob_grad, power))

        def third_stage(slot):
            pair, side = slot // 2, slot % 2
            count = distant + (side + 1) * rows
            q, g, probs, score_grad = held.pop(slot)
            if partial_only:
                outs[5][slot, :count] = probs
                outs[6][slot, :count] = score_grad
                wanted = order(0, rows)[0]
                accumulate(told, 0, contract(score_grad[wanted : wanted + rows], q, 1, 0))
                accumulate(told, 1, contract(probs[wanted : wanted + rows], g, 1, 0))
                return
            accumulate(dv, side, contract(probs, g, 1, 0))
            accumulate(dk, side, contract(score_grad, q, 1, 0))
            dq = (contract(keys_t[:, :count], score_grad, 1, 0) * scaling).T.astype(low)
            target = order(dq_own, dq_sib)[side]
            for member in range(2):
                at = (pair * 2 + member) * HD
                target[:, at : at + HD] = dq[member * rows : (member + 1) * rows]

        stages = (first_stage, second_stage, third_stage)
        for stage, slot in STAGGER:
            stages[stage](slot)
        if partial_only:
            out[:, :HD] = (told[0] * scaling).astype(low)
            out[:, HD:] = told[1].astype(low)
            return
        for slot, (lo, hi) in enumerate((dk, dv)):
            size = scaling if slot == 0 else 1.0
            spot = slice(slot * HD, (slot + 1) * HD)
            first, second = order(near_own, near_sib)
            first[:, spot] = (lo[distant:] + hi[distant : distant + rows]) * size
            second[:, spot] = hi[distant + rows :] * size
            if asks:
                out[:, spot] = ((lo[:distant] + hi[:distant]) * size).astype(low)

    specialise(place, body)
    if copies:
        for copy in copies:
            copy.wait()
        specialise(place, pass_on)


def settle_kernel(unit, place, own_all, sib_all, *refs):
    refs = list(refs)
    far = [refs.pop(0) for _ in range(unit["far"])]
    dq_own_in, dq_sib_in, near_own_in, near_sib_in, probs_in, grads_in = refs[:6]
    dq_own, back, near_own, out = refs[6:]
    rows = own_all.shape[0]
    group = QH // KVH
    scaling = 1.0 / math.sqrt(HD)
    low = jnp.bfloat16

    def body(asks, order):
        if not asks:
            dq_own[...] = dq_own_in[...]
            near_own[...] = near_own_in[...]
            back[:, : group * HD] = dq_sib_in[...]
            back[:, group * HD :] = near_sib_in[...].astype(low)
            return
        queries, grads, keys, _ = head_parts(asks, order, own_all, sib_all, far, unit["head"])
        keys_t = keys.T
        distant = 2 * rows
        dk, dv, told = [None, None], [None, None], [None, None]
        for pair in range(group // 2):
            for side in range(2):
                slot = pair * 2 + side
                count = distant + (side + 1) * rows
                q, g = queries(side, pair), grads(side, pair)
                probs, score_grad = probs_in[slot, :count], grads_in[slot, :count]
                wanted = order(0, rows)[1]
                accumulate(told, 0, contract(score_grad[wanted : wanted + rows], q, 1, 0))
                accumulate(told, 1, contract(probs[wanted : wanted + rows], g, 1, 0))
                accumulate(dv, side, contract(probs[distant:], g, 1, 0))
                accumulate(dk, side, contract(score_grad[distant:], q, 1, 0))
                dq = (contract(keys_t[:, :count], score_grad, 1, 0) * scaling).T.astype(low)
                target = order(dq_own, back)[side]
                for member in range(2):
                    at = (pair * 2 + member) * HD
                    target[:, at : at + HD] = dq[member * rows : (member + 1) * rows]
        for slot, (lo, hi) in enumerate((dk, dv)):
            size = scaling if slot == 0 else 1.0
            at = slot * HD
            targets = order((near_own, at), (back, group * HD + at))
            for (target, spot), value in zip(targets, (lo + hi[:rows], hi[rows:])):
                target[:, spot : spot + HD] = (value * size).astype(target.dtype)
            out[:, at : at + HD] = (told[slot] * size).astype(low)

    specialise(place, body)


def fold_kernel(count, place, *refs):
    nears, tolds, back = refs[:count], refs[count : 2 * count], refs[-1]
    core = place[0] % 2
    hears = place[0] // 2 == 0
    rows, width = nears[0].shape
    at = pl.multiple_of((1 - core) * rows, rows)
    for index in range(count):
        told = jnp.where(hears, tolds[index][pl.ds(at, rows), :].astype(jnp.float32), 0.0)
        back[:, index * width : (index + 1) * width] = (nears[index][...] + told).astype(back.dtype)


def join_kernel(plan, place, *refs):
    outs, (sums, sems) = refs[-5:-2], refs[-2:]
    core = place[0] % 2
    hears = place[0] // 2 == 0
    group = QH // KVH
    halves = [out.shape[1] // 2 for out in outs]
    rows = sums.shape[1]
    own_rows = pl.multiple_of(core * rows, HD)
    copies = []

    def write(source, out, start, width):
        target = out.at[:, pl.ds(pl.multiple_of(start, HD), width)]
        copies.append(pltpu.make_async_copy(source, target, sems.at[len(copies)]))
        copies[-1].start()

    def write_pair(source, at, head, owner):
        for slot in range(2):
            spot = slice(at + slot * HD, at + (slot + 1) * HD)
            write(source.at[:, spot], outs[1 + slot], owner * halves[1] + head * HD, HD)

    for head, own, other in plan["queries"]:
        width = group * HD
        write(refs[own], outs[0], core * halves[0] + head * width, width)
        write(refs[other].at[:, :width], outs[0], (1 - core) * halves[0] + head * width, width)
    for head, other, at in plan["ready"]:
        write_pair(refs[other], at, head, 1 - core)
    cell = 0
    for head, near, told, direct in plan["own"]:
        heard = refs[told][...] if direct else refs[told][pl.ds(own_rows, rows), :]
        total = refs[near][...] + jnp.where(hears, heard.astype(jnp.float32), 0.0)
        sums[cell] = total.astype(sums.dtype)
        write_pair(sums.at[cell], 0, head, core)
        cell += 1
    for head, other, at, told in plan["other"]:
        total = refs[other][:, at : at + 2 * HD].astype(jnp.float32)
        total = total + jnp.where(hears, refs[told][...].astype(jnp.float32), 0.0)
        sums[cell] = total.astype(sums.dtype)
        write_pair(sums.at[cell], 0, head, 1 - core)
        cell += 1
    for copy in copies:
        copy.wait()


def local_call(kernel, outs, args, scratch=(), flops=0, space=pltpu.VMEM, aliases=None, out_space=pltpu.VMEM, in_spaces=None):
    specs = [pl.BlockSpec(memory_space=pltpu.SMEM)]
    specs += [pl.BlockSpec(memory_space=kind) for kind in in_spaces or [space] * (len(args) - 1)]
    return pl.pallas_call(
        kernel,
        out_shape=tuple(outs),
        in_specs=specs,
        out_specs=tuple(pl.BlockSpec(memory_space=out_space) for _ in outs),
        scratch_shapes=scratch,
        input_output_aliases=aliases or {},
        compiler_params=pltpu.CompilerParams(vmem_limit_bytes=VMEM_BYTES),
        cost_estimate=pl.CostEstimate(flops=flops, transcendentals=0, bytes_accessed=0),
    )(*args)


def plan_units():
    count = KVH // 2
    return [
        {
            "head": head,
            "far": 2 if head < LAG else 1,
            "told": 2 if head == count - 1 else 1,
            "later": head + LAG if head + LAG < count else None,
        }
        for head in range(count)
    ]


def on_pair(query_rows, key_rows, value_rows, out_grad, question_lengths):
    rows = query_rows.shape[0]
    group = QH // KVH
    low = jnp.bfloat16
    full = jnp.float32
    shape = jax.ShapeDtypeStruct
    units = plan_units()
    count = len(units)
    sib = [(0, 1), (1, 0), (2, 3), (3, 2)]
    same = [(0, 2), (1, 3), (2, 0), (3, 1)]
    cross = [(0, 3), (1, 2), (2, 1), (3, 0)]
    link = shape((rows, 2 * HD), low)
    wide = shape((rows, query_rows.shape[1] + key_rows.shape[1]), low)
    block = shape((group, 4 * rows, 2 * rows), low)

    def send(value, perm):
        return lax.ppermute(value, "sp", perm)

    place = lax.axis_index("sp").astype(jnp.int32).reshape(1)
    whole = (query_rows, out_grad, key_rows, value_rows, question_lengths)
    fixed = tuple(pltpu.with_memory_space_constraint(value, pltpu.HBM) for value in whole)
    narrow = shape((rows, 2 * (group + 1) * HD), low)
    lent = [wide, narrow, shape((2 * rows, 2 * rows), full)]
    *packs, sib_send, own_first, bias = local_call(
        pack_kernel, [link] * (2 * LAG) + lent, (place, *fixed[:4]), space=pltpu.HBM,
        scratch=[pltpu.SemaphoreType.DMA((4 * LAG + 8,))],
    )
    args = (place, *fixed, sib_send, own_first, bias)
    sib_send, own_first, bias = local_call(
        lend_kernel, lent, args, aliases={6 + i: i for i in range(3)},
        in_spaces=[pltpu.HBM] * 5 + [pltpu.VMEM] * 3,
        scratch=[
            pltpu.SMEM(question_lengths.shape, jnp.int32), pltpu.SemaphoreType.DMA((9,)),
        ],
    )
    far = []
    for chunk in range(LAG):
        far.append((send(packs[2 * chunk], same), send(packs[2 * chunk + 1], cross)))
    sib_all = send(sib_send, sib)
    wings = [shape((rows, group * HD), low)] * 2
    near = shape((rows, 2 * HD), full)
    dq_own, dq_sib, near_own, near_sib = [], [], [], []
    for index, unit in enumerate(units):
        split = unit["told"] == 2
        lead = index == 0
        args = (place, bias, own_first if lead else own_all, sib_all, *far[index])
        outs = local_call(
            partial(attend_kernel, unit),
            [*wings, near, near, link if split else shape((2 * rows, 2 * HD), low)]
            + ([block, block] if split else []) + ([wide] if lead else []),
            args + (fixed[:4] if lead else ()),
            in_spaces=[pltpu.VMEM] * (len(args) - 1) + [pltpu.HBM] * (4 if lead else 0),
            scratch=[pltpu.SemaphoreType.DMA((4,))] if lead else (),
            flops=group * 10 * HD * 2 * rows * 4 * rows,
        )
        if lead:
            own_all = outs[5]
        told = send(outs[4], same)
        if split:
            outs = local_call(
                partial(settle_kernel, unit),
                [wings[0], shape((rows, (group + 2) * HD), low), near, link],
                (place, own_all, sib_all, *far[index], *outs[:4], *outs[5:]),
                flops=group * 4 * HD * 2 * rows * 4 * rows,
            )
            told_cross = send(outs[3], cross)
            back_last = send(outs[1], sib)
            dq_last, near_last, told_last = outs[0], outs[2], told
        else:
            far.append((told,))
            dq_own.append(outs[0])
            dq_sib.append(send(outs[1], sib))
            near_own.append(outs[2])
            near_sib.append(outs[3])
    heard = [value[0] for value in far[LAG:]]
    shapes = [shape(value.shape, low) for value in (query_rows, key_rows, value_rows)]
    ready, head = [], 0
    for size in FOLDS:
        span = slice(head, head + size)
        folded, = local_call(
            partial(fold_kernel, size), [shape((rows, size * 2 * HD), low)],
            (place, *near_sib[span], *heard[span]),
        )
        folded = send(folded, sib)
        ready.append([(head + i, folded, 2 * i * HD) for i in range(size)])
        head += size

    def join(results, queries, own, ready, other):
        args = []

        def use(value):
            args.append(value)
            return len(args) - 1

        plan = {
            "queries": [(at, use(first), use(second)) for at, first, second in queries],
            "ready": [(at, use(value), spot) for at, value, spot in ready],
            "own": [(at, use(near), use(told), direct) for at, near, told, direct in own],
            "other": [(at, use(value), spot, use(told)) for at, value, spot, told in other],
        }
        cells = len(own) + len(other)
        writes = 2 * (len(queries) + len(ready) + cells)
        return local_call(
            partial(join_kernel, plan), shapes, (place, *args, *results),
            aliases={1 + len(args) + i: i for i in range(len(results))},
            in_spaces=[pltpu.VMEM] * len(args) + [pltpu.HBM] * len(results),
            out_space=pltpu.HBM,
            scratch=[pltpu.VMEM((cells, rows, 2 * HD), low), pltpu.SemaphoreType.DMA((writes,))],
        )

    last = count - 1
    queries = [(i, dq_own[i], dq_sib[i]) for i in range(last)]
    own = [(i, near_own[i], heard[i], False) for i in range(last)]
    soon = sum(FOLDS[:-1])
    results = join(
        (), queries + [(last, dq_last, back_last)], own[:soon], [item for part in ready[:-1] for item in part], ()
    )
    results = join(
        results, (),
        own[soon:] + [(last, near_last, told_last, True)], ready[-1],
        [(last, back_last, group * HD, told_cross)],
    )
    return tuple(results)


def solution(mesh):
    paired = mesh.shape["sp"] == 4
    rows = P(("grp", "sp"), None)
    return jax.shard_map(
        on_pair if paired else on_device,
        mesh=mesh,
        in_specs=(rows, rows, rows, rows, P("grp")),
        out_specs=(rows, rows, rows),
        check_vma=False,
    )
```
